32 devices in a mesh: row: 4 (over y, core), col: 8 (over z, x).
Axes of the slice: x: 2, y: 2, z: 4, core: 2. Of those that a mesh axis runs over, the one named last changes fastest.
Arguments:
- lhat: float32 [256, 256, 256], P(('row', 'col')), may hold values from -0.375 to 0.375
- ainv_anc: float32 [256, 256, 256], P(('row', 'col')), may hold values from -2.5 to 2.5
- diag_inv: float32 [8, 256, 256], P('col', 'row'), may hold values from -0.6 to 2, as said below
- targets: int32 [256, 1], P(('row', 'col')), may hold values from 0 to 7
Outputs:
- diag_blocks: float32 [8, 256, 256], P('col', 'row')
The draws below stay inside these ranges and needn't reach their ends.
Inputs may be any that keep to these rules, and one draw needn't show every extreme that they name: `diag_inv`: each block is lower triangular with its diagonal entries between 0.5 and 2.
All inputs are finite; a program needn't handle non-finite values.
Results may differ from the reference program's by a relative error of at most 0.0003.
Values sent between devices are 32-bit elements; how exact they have to be, the bound alone decides.
A program may use at most 64 MiB of HBM per device.

```python
import jax
import jax.numpy as jnp
from jax import lax

W = 256
H = 256
SN_DEV = 1
SLOT_DEV = 8
SUPER = 8
SLOTS = 256
N_ROW = 4
N_COL = 8


def draw_diag_inv(key, part):
    first, second = jax.random.split(jax.random.fold_in(key, 17))
    spread = 0.1 * jax.random.normal(first, (SUPER, W, W), jnp.float32)
    spread = jnp.clip(spread, -0.6, 0.6)
    diagonal = jax.random.uniform(second, (SUPER, W), jnp.float32, 0.5, 2.0)
    lower = jnp.tril(spread, -1)
    return lower + diagonal[:, :, None] * jnp.eye(W, dtype=jnp.float32)[None, :, :]


def steps_of(key, extent, shards, least, high):
    factor_of = 1.0
    for dim, shards_of in shards:
        heights = jax.random.uniform(jax.random.fold_in(jax.random.fold_in(key, 6), dim), (shards_of,), jnp.float32, least / len(shards), high / len(shards))
        factor_of = factor_of * jnp.repeat(jnp.exp(heights), extent[dim] // shards_of).reshape((-1,) + (1,) * (len(extent) - 1 - dim))
    return factor_of


def picks_of(own_key, rows, number_of, top, lift):
    ranking = jax.random.permutation(jax.random.fold_in(own_key, 1), number_of)
    boost = ranking
    for power in range(3):
        boost = boost * boost // number_of
    boost = boost * lift // number_of
    tickets = jax.random.randint(jax.random.fold_in(own_key, 2), (rows, number_of), 0, 4096) + boost
    sure = jax.random.permutation(jax.random.fold_in(own_key, 3), rows)[jnp.arange(number_of) % rows]
    tickets = jnp.where(jnp.arange(rows)[:, None] == sure[None, :], 1 << 14, tickets)
    priority = tickets * number_of + jnp.arange(number_of)
    return lax.top_k(priority.astype(jnp.int32), top)[1].astype(jnp.int32)


def normal_values(stream_key, extent, width, bound, shards=(), held_as=jnp.bfloat16):
    drawn = width * jax.random.normal(stream_key, extent, jnp.float32)
    if shards:
        drawn = drawn * steps_of(stream_key, extent, shards, -0.22, 0.18)
    return jnp.clip(drawn, -bound, bound).astype(held_as)


def setup_inputs(seed: int = 0) -> dict:
    key_of = jax.random.split(jax.random.key(seed), 5)
    lhat = normal_values(key_of[0], (SLOTS, H, W), H ** -0.5, 0.375, ((0, 32),), jnp.float32)
    ainv_anc = normal_values(key_of[1], (SLOTS, H, W), ((SN_DEV / (SLOT_DEV * N_ROW)) ** 0.5), 2.5, ((0, 32),), jnp.float32)
    diag_inv = draw_diag_inv(jax.random.fold_in(key_of[4], 71), 0)
    targets = picks_of(key_of[3], SLOTS, SUPER, 1, 2048)
    return dict(lhat=lhat, ainv_anc=ainv_anc, diag_inv=diag_inv, targets=targets)


def reference(lhat, ainv_anc, diag_inv, targets):
    group_size = SLOT_DEV * N_COL
    slot_ids = targets[:, 0].reshape(N_ROW, group_size)
    left_all = lhat.reshape(N_ROW, group_size, H, W)
    right_all = ainv_anc.reshape(N_ROW, group_size, H, W)
    labels = jnp.arange(SN_DEV * N_COL, dtype=jnp.int32)

    def accumulate(running, inputs):
        left_blk, right_blk, ids_blk = inputs
        products = jnp.einsum('shi,shj->sij', left_blk, right_blk, precision=lax.Precision.HIGHEST)
        one_hot = (labels[:, None] == ids_blk[None, :]).astype(jnp.float32)
        added = jnp.einsum('ks,sij->kij', one_hot, products, precision=lax.Precision.HIGHEST)
        return running + added, None

    start_sum = jnp.zeros((SN_DEV * N_COL, W, W), jnp.float32)
    contrib, leftover = lax.scan(accumulate, start_sum, (left_all, right_all, slot_ids))
    gram_term = jnp.einsum('kia,kib->kab', diag_inv, diag_inv, precision=lax.Precision.HIGHEST)
    return gram_term - contrib
```

```python
import functools

import jax
import jax.numpy as jnp
from jax import lax
from jax.experimental import pallas as pl
from jax.experimental.pallas import tpu as pltpu
from jax.sharding import PartitionSpec as P

MESH = pl.DeviceIdType.MESH
DN = (((0,), (0,)), ((), ()))


def gram_dot(a, b):
    a_hi = a.astype(jnp.bfloat16)
    a_lo = (a - a_hi.astype(jnp.float32)).astype(jnp.bfloat16)
    b_hi = b.astype(jnp.bfloat16)
    b_lo = (b - b_hi.astype(jnp.float32)).astype(jnp.bfloat16)
    left = jnp.concatenate([a_hi, a_lo, a_hi], axis=0)
    right = jnp.concatenate([b_hi, b_hi, b_lo], axis=0)
    return lax.dot_general(left, right, DN, preferred_element_type=jnp.float32)


def kernel(
    dims,
    lhat, ainv, diag, targets_in, out,
    targets, lbuf, abuf, dbuf, prod, cum, send0, recv0, send1a, send1b, recv1a, recv1b,
    sum2a, sum2b, recv2a, recv2b, sum3, recv3,
    load_sem, d_sem, t_sem, relay, s0, r0, s1a, r1a, s1b, r1b, s2a, r2a, s2b, r2b, s3, r3,
):
    yn, zn, slots, share, width = dims
    half = width // 2
    row, col = lax.axis_index("row"), lax.axis_index("col")
    y, c = lax.div(row, 2), lax.rem(row, 2)
    z, x = lax.div(col, 2), lax.rem(col, 2)

    def dev(y_, c_, z_, x_):
        return {"row": y_ * 2 + c_, "col": z_ * 2 + x_}

    shifts = [zn // 2] + [d for d in range(1, zn) if d != zn // 2] if zn > 1 else []
    order = shifts + [0]
    core_peer = dev(y, 1 - c, z, x)
    x_peer = dev(y, c, z, 1 - x)
    y_ids = [lax.rem(y + d, yn) for d in range(1, yn)]
    y_peers = [dev(i, c, z, x) for i in y_ids]
    z_peers = [dev(y, c, lax.rem(z + d, zn), x) for d in shifts]
    z_near = [dev(y, c, lax.rem(z + d, zn), x) for d in {1 % zn, (zn - 1) % zn} - {0}]
    near = [core_peer, x_peer] + y_peers + z_near
    prev_z = dev(y, c, lax.rem(z + zn - 1, zn), x)

    t_load = pltpu.make_async_copy(targets_in, targets, t_sem)
    t_load.start()
    d_load = pltpu.make_async_copy(diag.at[0], dbuf, d_sem)
    d_load.start()
    loads = []
    for s in range(slots):
        pair = (
            pltpu.make_async_copy(lhat.at[s], lbuf.at[s], load_sem.at[s, 0]),
            pltpu.make_async_copy(ainv.at[s], abuf.at[s], load_sem.at[s, 1]),
        )
        for copy in pair:
            copy.start()
        loads.append(pair)

    barrier = pltpu.get_barrier_semaphore()
    for peer in near:
        pl.semaphore_signal(barrier, inc=1, device_id=peer, device_id_type=MESH)

    t_load.wait()
    ids = [targets[0, s] for s in range(slots)] + [col]
    count = len(ids)

    def less(k):
        total = jnp.int32(0)
        for t in ids:
            total = total + (t < k).astype(jnp.int32)
        return total

    ranks = []
    for s in range(count):
        rank = jnp.int32(0)
        for r in range(count):
            ahead = ids[r] <= ids[s] if r < s else ids[r] < ids[s]
            if r != s:
                rank = rank + ahead.astype(jnp.int32)
        ranks.append(rank)
    sorted_slots = []
    for j in range(count):
        slot = jnp.int32(0)
        for s in range(1, count):
            slot = slot + jnp.where(ranks[s] == j, s, 0)
        sorted_slots.append(slot)

    d_load.wait()
    prod[slots] = -gram_dot(dbuf[...], dbuf[...]).reshape(yn, 2, share, width)
    first = 0
    for group in (1, slots - 1):
        for s in range(first, first + group):
            for copy in loads[s]:
                copy.wait()
        for s in range(first, first + group):
            prod[s] = gram_dot(lbuf[s], abuf[s]).reshape(yn, 2, share, width)
        first += group

    def prefix(side):
        for yo in range(yn):
            cum[0, yo, side] = jnp.zeros((share, width), jnp.float32)
            total = prod[sorted_slots[0], yo, side]
            cum[1, yo, side] = total
            for j in range(1, count):
                total = total + prod[sorted_slots[j], yo, side]
                cum[j + 1, yo, side] = total

    bounds = {}
    for o in range(zn):
        for xi in range(2):
            k = lax.rem(z + order[o], zn) * 2 + xi
            bounds[o, xi] = (less(k), less(k + 1))

    def part(o, h, xi, yo, side):
        lanes = slice(h * half, (h + 1) * half)
        begin, end = bounds[o, xi]
        return cum[begin, yo, side, :, lanes] - cum[end, yo, side, :, lanes]

    def dynamic_part(o, h, xi, yo):
        lanes = slice(h * half, (h + 1) * half)
        begin = jnp.where(xi == 0, bounds[o, 0][0], bounds[o, 1][0])
        end = jnp.where(xi == 0, bounds[o, 0][1], bounds[o, 1][1])
        return cum[begin, yo, c, :, lanes] - cum[end, yo, c, :, lanes]

    def segment(o):
        for xi in range(2):
            for yo in range(yn):
                for h in range(2):
                    send0[o, h, xi, yo] = part(o, h, xi, yo, 1 - c)

    def remote(src, dst, send, recv, peer):
        copy = pltpu.make_async_remote_copy(
            src_ref=src, dst_ref=dst, send_sem=send, recv_sem=recv, device_id=peer, device_id_type=MESH
        )
        copy.start()
        return copy

    started = []
    copies0, copies1a, copies1b, copies2a, copies2b = {}, {}, {}, {}, {}
    copies3 = {}

    def stage0(o):
        copies0[o] = remote(send0.at[o], recv0.at[o], s0.at[o], r0.at[o], core_peer)
        started.append(copies0[o])

    def stage1(o):
        copies0[o].wait_recv()
        for yo in range(yn):
            send1a[o, yo] = dynamic_part(o, 0, 1 - x, yo) + recv0[o, 0, 1 - x, yo]
        for i, yo in enumerate(y_ids):
            for xi in range(2):
                send1b[o, i, xi] = part(o, 1, xi, yo, c) + recv0[o, 1, xi, yo]
        copies1a[o] = remote(send1a.at[o], recv1a.at[o], s1a.at[o], r1a.at[o], x_peer)
        copies1b[o] = [
            remote(send1b.at[o, i], recv1b.at[o, i], s1b.at[o, i], r1b.at[o, i], peer)
            for i, peer in enumerate(y_peers)
        ]
        started.extend([copies1a[o]] + copies1b[o])

    def stage2(o):
        copies1a[o].wait_recv()
        for yo in range(yn):
            sum2a[o, yo] = dynamic_part(o, 0, x, yo) + recv0[o, 0, x, yo] + recv1a[o, yo]
        copies2a[o] = [
            remote(sum2a.at[o, yo], recv2a.at[o, i], s2a.at[o, i], r2a.at[o, i], peer)
            for i, (yo, peer) in enumerate(zip(y_ids, y_peers))
        ]
        for copy in copies1b[o]:
            copy.wait_recv()
        for xi in range(2):
            total = part(o, 1, xi, y, c) + recv0[o, 1, xi, y]
            for i in range(yn - 1):
                total = total + recv1b[o, i, xi]
            sum2b[o, xi] = total
        copies2b[o] = remote(sum2b.at[o, 1 - x], recv2b.at[o], s2b.at[o], r2b.at[o], x_peer)
        started.extend(copies2a[o] + [copies2b[o]])

    def stage3(o):
        for copy in copies2a[o]:
            copy.wait_recv()
        total = sum2a[o, y]
        for i in range(yn - 1):
            total = total + recv2a[o, i]
        sum3[o, 0] = total
        if o < zn - 1:
            first = remote(sum3.at[o, 0], recv3.at[o, 0], s3.at[o, 0], r3.at[o, 0], z_peers[o])
        copies2b[o].wait_recv()
        sum3[o, 1] = sum2b[o, x] + recv2b[o]
        if o < zn - 1:
            second = remote(sum3.at[o, 1], recv3.at[o, 1], s3.at[o, 1], r3.at[o, 1], z_peers[o])
            copies3[o] = (first, second)
            started.extend(copies3[o])

    prefix(1 - c)
    for o in range(zn):
        segment(o)
        if o == 0:
            pl.semaphore_wait(barrier, len(near))
        stage0(o)
    if zn > 2:
        pl.semaphore_signal(relay, inc=1, device_id=prev_z, device_id_type=MESH)
    prefix(c)
    ahead, lag = 2, 2
    for step in range(zn + ahead + lag):
        if step < zn:
            stage1(step)
        if step == ahead + lag and zn > 2:
            pl.semaphore_wait(relay, 1)
        if 0 <= step - ahead < zn:
            stage2(step - ahead)
        if 0 <= step - ahead - lag < zn:
            stage3(step - ahead - lag)

    totals = [sum3[zn - 1, h] for h in range(2)]
    for o in range(zn - 1):
        for h in range(2):
            copies3[o][h].wait_recv()
            totals[h] = totals[h] + recv3[o, h]
    for h in range(2):
        out[0, :, h * half:(h + 1) * half] = totals[h]
    for copy in started:
        copy.wait_send()


def on_device(lhat, ainv, diag, targets):
    rows, cols = lax.axis_size("row"), lax.axis_size("col")
    slots, width = lhat.shape[0], lhat.shape[2]
    height = lhat.shape[1]
    yn, zn, share = rows // 2, cols // 2, diag.shape[1]
    half = width // 2
    f32, dma = jnp.float32, pltpu.SemaphoreType.DMA
    tail = (share, half)
    scratch = [
        pltpu.SMEM((1, slots), jnp.int32),
        pltpu.VMEM((slots, height, width), f32),
        pltpu.VMEM((slots, height, width), f32),
        pltpu.VMEM((share, width), f32),
        pltpu.VMEM((slots + 1, yn, 2, share, width), f32),
        pltpu.VMEM((slots + 2, yn, 2, share, width), f32),
        pltpu.VMEM((zn, 2, 2, yn) + tail, f32),
        pltpu.VMEM((zn, 2, 2, yn) + tail, f32),
        pltpu.VMEM((zn, yn) + tail, f32),
        pltpu.VMEM((zn, yn - 1, 2) + tail, f32),
        pltpu.VMEM((zn, yn) + tail, f32),
        pltpu.VMEM((zn, yn - 1, 2) + tail, f32),
        pltpu.VMEM((zn, yn) + tail, f32),
        pltpu.VMEM((zn, 2) + tail, f32),
        pltpu.VMEM((zn, yn - 1) + tail, f32),
        pltpu.VMEM((zn,) + tail, f32),
        pltpu.VMEM((zn, 2) + tail, f32),
        pltpu.VMEM((zn - 1, 2) + tail, f32),
        dma((slots, 2)), dma, dma, pltpu.SemaphoreType.REGULAR,
        dma((zn,)), dma((zn,)),
        dma((zn,)), dma((zn,)),
        dma((zn, yn - 1)), dma((zn, yn - 1)),
        dma((zn, yn - 1)), dma((zn, yn - 1)),
        dma((zn,)), dma((zn,)),
        dma((zn - 1, 2)), dma((zn - 1, 2)),
    ]
    return pl.pallas_call(
        functools.partial(kernel, (yn, zn, slots, share, width)),
        out_shape=pltpu.VMEM(diag.shape, f32),
        in_specs=[pl.BlockSpec(memory_space=pltpu.HBM)] * 4,
        out_specs=pl.BlockSpec(memory_space=pltpu.VMEM),
        scratch_shapes=scratch,
        compiler_params=pltpu.CompilerParams(
            collective_id=0, has_side_effects=True, vmem_limit_bytes=60 * 1024 * 1024
        ),
    )(lhat, ainv, diag, targets.T)


def solution(mesh):
    placed = (
        P(("row", "col"), None, None),
        P(("row", "col"), None, None),
        P("col", "row", None),
        P(("row", "col"), None),
    )
    return jax.shard_map(
        on_device, mesh=mesh, in_specs=placed, out_specs=P("col", "row", None), check_vma=False
    )
```

```python
import functools

import jax
import jax.numpy as jnp
from jax import lax
from jax.experimental import pallas as pl
from jax.experimental.pallas import tpu as pltpu
from jax.sharding import PartitionSpec as P

MESH = pl.DeviceIdType.MESH
DN = (((0,), (0,)), ((), ()))


def gram_dot(a, b):
    a_hi = a.astype(jnp.bfloat16)
    a_lo = (a - a_hi.astype(jnp.float32)).astype(jnp.bfloat16)
    b_hi = b.astype(jnp.bfloat16)
    b_lo = (b - b_hi.astype(jnp.float32)).astype(jnp.bfloat16)
    left = jnp.concatenate([a_hi, a_lo, a_hi], axis=0)
    right = jnp.concatenate([b_hi, b_hi, b_lo], axis=0)
    return lax.dot_general(left, right, DN, preferred_element_type=jnp.float32)


def kernel(
    dims,
    lhat, ainv, diag, targets_in, out,
    targets, lbuf, abuf, dbuf, prod, cum, send0, recv0, send1a, send1b, recv1a, recv1b,
    sum2a, sum2b, recv2a, recv2b, sum3, recv3,
    load_sem, d_sem, t_sem, relay, s0, r0, s1a, r1a, s1b, r1b, s2a, r2a, s2b, r2b, s3, r3,
):
    yn, zn, slots, share, width = dims
    half = width // 2
    row, col = lax.axis_index("row"), lax.axis_index("col")
    y, c = lax.div(row, 2), lax.rem(row, 2)
    z, x = lax.div(col, 2), lax.rem(col, 2)

    def dev(y_, c_, z_, x_):
        return {"row": y_ * 2 + c_, "col": z_ * 2 + x_}

    order = [jnp.where(o < z, o, o + 1) for o in range(zn - 1)] + [z]
    core_peer = dev(y, 1 - c, z, x)
    x_peer = dev(y, c, z, 1 - x)
    y_ids = [lax.rem(y + d, yn) for d in range(1, yn)]
    y_peers = [dev(i, c, z, x) for i in y_ids]
    z_peers = [dev(y, c, zd, x) for zd in order[:-1]]
    z_slots = [jnp.where(z < zd, z, z - 1) for zd in order[:-1]]
    z_near = [dev(y, c, lax.rem(z + d, zn), x) for d in {1 % zn, (zn - 1) % zn} - {0}]
    near = [core_peer, x_peer] + y_peers + z_near
    prev_z = dev(y, c, lax.rem(z + zn - 1, zn), x)

    t_load = pltpu.make_async_copy(targets_in, targets, t_sem)
    t_load.start()
    d_load = pltpu.make_async_copy(diag.at[0], dbuf, d_sem)
    d_load.start()
    loads = []
    for s in range(slots):
        pair = (
            pltpu.make_async_copy(lhat.at[s], lbuf.at[s], load_sem.at[s, 0]),
            pltpu.make_async_copy(ainv.at[s], abuf.at[s], load_sem.at[s, 1]),
        )
        for copy in pair:
            copy.start()
        loads.append(pair)

    barrier = pltpu.get_barrier_semaphore()
    for peer in near:
        pl.semaphore_signal(barrier, inc=1, device_id=peer, device_id_type=MESH)

    for copy in loads[0]:
        copy.wait()
    prod[0] = gram_dot(lbuf[0], abuf[0]).reshape(yn, 2, share, width)
    for s in range(1, slots):
        for copy in loads[s]:
            copy.wait()
    d_load.wait()
    t_load.wait()
    ids = [targets[0, s] for s in range(slots)] + [col]
    count = len(ids)

    def less(k):
        total = jnp.int32(0)
        for t in ids:
            total = total + (t < k).astype(jnp.int32)
        return total

    ranks = []
    for s in range(count):
        rank = jnp.int32(0)
        for r in range(count):
            ahead = ids[r] <= ids[s] if r < s else ids[r] < ids[s]
            if r != s:
                rank = rank + ahead.astype(jnp.int32)
        ranks.append(rank)
    sorted_slots = []
    for j in range(count):
        slot = jnp.int32(0)
        for s in range(1, count):
            slot = slot + jnp.where(ranks[s] == j, s, 0)
        sorted_slots.append(slot)

    for s in range(1, slots):
        prod[s] = gram_dot(lbuf[s], abuf[s]).reshape(yn, 2, share, width)
    prod[slots] = -gram_dot(dbuf[...], dbuf[...]).reshape(yn, 2, share, width)

    def prefix(side):
        for yo in range(yn):
            cum[0, yo, side] = jnp.zeros((share, width), jnp.float32)
            total = prod[sorted_slots[0], yo, side]
            cum[1, yo, side] = total
            for j in range(1, count):
                total = total + prod[sorted_slots[j], yo, side]
                cum[j + 1, yo, side] = total

    bounds = {}
    for o in range(zn):
        for xi in range(2):
            k = order[o] * 2 + xi
            bounds[o, xi] = (less(k), less(k + 1))

    def part(o, h, xi, yo, side):
        lanes = slice(h * half, (h + 1) * half)
        begin, end = bounds[o, xi]
        return cum[begin, yo, side, :, lanes] - cum[end, yo, side, :, lanes]

    def dynamic_part(o, h, xi, yo):
        lanes = slice(h * half, (h + 1) * half)
        begin = jnp.where(xi == 0, bounds[o, 0][0], bounds[o, 1][0])
        end = jnp.where(xi == 0, bounds[o, 0][1], bounds[o, 1][1])
        return cum[begin, yo, c, :, lanes] - cum[end, yo, c, :, lanes]

    def segment(o):
        for xi in range(2):
            for yo in range(yn):
                for h in range(2):
                    send0[o, h, xi, yo] = part(o, h, xi, yo, 1 - c)

    def remote(src, dst, send, recv, peer):
        copy = pltpu.make_async_remote_copy(
            src_ref=src, dst_ref=dst, send_sem=send, recv_sem=recv, device_id=peer, device_id_type=MESH
        )
        copy.start()
        return copy

    started = []
    copies0, copies1a, copies1b, copies2a, copies2b = {}, {}, {}, {}, {}
    copies3 = {}

    def stage0(o):
        copies0[o] = remote(send0.at[o], recv0.at[o], s0.at[o], r0.at[o], core_peer)
        started.append(copies0[o])

    def stage1(o):
        copies0[o].wait_recv()
        for yo in range(yn):
            send1a[o, yo] = dynamic_part(o, 0, 1 - x, yo) + recv0[o, 0, 1 - x, yo]
        for i, yo in enumerate(y_ids):
            for xi in range(2):
                send1b[o, i, xi] = part(o, 1, xi, yo, c) + recv0[o, 1, xi, yo]
        copies1a[o] = remote(send1a.at[o], recv1a.at[o], s1a.at[o], r1a.at[o], x_peer)
        copies1b[o] = [
            remote(send1b.at[o, i], recv1b.at[o, i], s1b.at[o, i], r1b.at[o, i], peer)
            for i, peer in enumerate(y_peers)
        ]
        started.extend([copies1a[o]] + copies1b[o])

    def stage2(o):
        copies1a[o].wait_recv()
        for yo in range(yn):
            sum2a[o, yo] = dynamic_part(o, 0, x, yo) + recv0[o, 0, x, yo] + recv1a[o, yo]
        copies2a[o] = [
            remote(sum2a.at[o, yo], recv2a.at[o, i], s2a.at[o, i], r2a.at[o, i], peer)
            for i, (yo, peer) in enumerate(zip(y_ids, y_peers))
        ]
        for copy in copies1b[o]:
            copy.wait_recv()
        for xi in range(2):
            total = part(o, 1, xi, y, c) + recv0[o, 1, xi, y]
            for i in range(yn - 1):
                total = total + recv1b[o, i, xi]
            sum2b[o, xi] = total
        copies2b[o] = remote(sum2b.at[o, 1 - x], recv2b.at[o], s2b.at[o], r2b.at[o], x_peer)
        started.extend(copies2a[o] + [copies2b[o]])

    def stage3(o):
        for copy in copies2a[o]:
            copy.wait_recv()
        total = sum2a[o, y]
        for i in range(yn - 1):
            total = total + recv2a[o, i]
        sum3[o, 0] = total
        if o < zn - 1:
            first = remote(sum3.at[o, 0], recv3.at[z_slots[o], 0], s3.at[o, 0], r3.at[z_slots[o], 0], z_peers[o])
        copies2b[o].wait_recv()
        sum3[o, 1] = sum2b[o, x] + recv2b[o]
        if o < zn - 1:
            second = remote(sum3.at[o, 1], recv3.at[z_slots[o], 1], s3.at[o, 1], r3.at[z_slots[o], 1], z_peers[o])
            copies3[o] = (first, second)
            started.extend(copies3[o])

    prefix(1 - c)
    for o in range(zn):
        segment(o)
        if o == 0:
            pl.semaphore_wait(barrier, len(near))
        stage0(o)
    if zn > 2:
        pl.semaphore_signal(relay, inc=1, device_id=prev_z, device_id_type=MESH)
    prefix(c)
    ahead, lag = 2, 2
    for step in range(zn + ahead + lag):
        if step < zn:
            stage1(step)
        if step == ahead + lag and zn > 2:
            pl.semaphore_wait(relay, 1)
        if 0 <= step - ahead < zn:
            stage2(step - ahead)
        if 0 <= step - ahead - lag < zn:
            stage3(step - ahead - lag)

    def incoming(i, h):
        return pltpu.make_async_remote_copy(
            src_ref=recv3.at[i, h], dst_ref=recv3.at[i, h], send_sem=s3.at[i, h], recv_sem=r3.at[i, h],
            device_id=core_peer, device_id_type=MESH,
        )

    totals = [sum3[zn - 1, h] for h in range(2)]
    for o in range(zn - 1):
        for h in range(2):
            incoming(o, h).wait_recv()
            totals[h] = totals[h] + recv3[o, h]
    for h in range(2):
        out[0, :, h * half:(h + 1) * half] = totals[h]
    for copy in started:
        copy.wait_send()


def on_device(lhat, ainv, diag, targets):
    rows, cols = lax.axis_size("row"), lax.axis_size("col")
    slots, width = lhat.shape[0], lhat.shape[2]
    height = lhat.shape[1]
    yn, zn, share = rows // 2, cols // 2, diag.shape[1]
    half = width // 2
    f32, dma = jnp.float32, pltpu.SemaphoreType.DMA
    tail = (share, half)
    scratch = [
        pltpu.SMEM((1, slots), jnp.int32),
        pltpu.VMEM((slots, height, width), f32),
        pltpu.VMEM((slots, height, width), f32),
        pltpu.VMEM((share, width), f32),
        pltpu.VMEM((slots + 1, yn, 2, share, width), f32),
        pltpu.VMEM((slots + 2, yn, 2, share, width), f32),
        pltpu.VMEM((zn, 2, 2, yn) + tail, f32),
        pltpu.VMEM((zn, 2, 2, yn) + tail, f32),
        pltpu.VMEM((zn, yn) + tail, f32),
        pltpu.VMEM((zn, yn - 1, 2) + tail, f32),
        pltpu.VMEM((zn, yn) + tail, f32),
        pltpu.VMEM((zn, yn - 1, 2) + tail, f32),
        pltpu.VMEM((zn, yn) + tail, f32),
        pltpu.VMEM((zn, 2) + tail, f32),
        pltpu.VMEM((zn, yn - 1) + tail, f32),
        pltpu.VMEM((zn,) + tail, f32),
        pltpu.VMEM((zn, 2) + tail, f32),
        pltpu.VMEM((zn - 1, 2) + tail, f32),
        dma((slots, 2)), dma, dma, pltpu.SemaphoreType.REGULAR,
        dma((zn,)), dma((zn,)),
        dma((zn,)), dma((zn,)),
        dma((zn, yn - 1)), dma((zn, yn - 1)),
        dma((zn, yn - 1)), dma((zn, yn - 1)),
        dma((zn,)), dma((zn,)),
        dma((zn - 1, 2)), dma((zn - 1, 2)),
    ]
    return pl.pallas_call(
        functools.partial(kernel, (yn, zn, slots, share, width)),
        out_shape=pltpu.VMEM(diag.shape, f32),
        in_specs=[pl.BlockSpec(memory_space=pltpu.HBM)] * 4,
        out_specs=pl.BlockSpec(memory_space=pltpu.VMEM),
        scratch_shapes=scratch,
        compiler_params=pltpu.CompilerParams(
            collective_id=0, has_side_effects=True, vmem_limit_bytes=60 * 1024 * 1024
        ),
    )(lhat, ainv, diag, targets.T)


def solution(mesh):
    placed = (
        P(("row", "col"), None, None),
        P(("row", "col"), None, None),
        P("col", "row", None),
        P(("row", "col"), None),
    )
    return jax.shard_map(
        on_device, mesh=mesh, in_specs=placed, out_specs=P("col", "row", None), check_vma=False
    )
```

```python
import functools

import jax
import jax.numpy as jnp
from jax import lax
from jax.experimental import pallas as pl
from jax.experimental.pallas import tpu as pltpu
from jax.sharding import PartitionSpec as P

MESH = pl.DeviceIdType.MESH
DN = (((0,), (0,)), ((), ()))


def gram_dot(a, b):
    a_hi = a.astype(jnp.bfloat16)
    a_lo = (a - a_hi.astype(jnp.float32)).astype(jnp.bfloat16)
    b_hi = b.astype(jnp.bfloat16)
    b_lo = (b - b_hi.astype(jnp.float32)).astype(jnp.bfloat16)
    left = jnp.concatenate([a_hi, a_lo, a_hi], axis=0)
    right = jnp.concatenate([b_hi, b_hi, b_lo], axis=0)
    return lax.dot_general(left, right, DN, preferred_element_type=jnp.float32)


def top_rows(share):
    return share // 4 // 8 * 8


def kernel(
    dims,
    lhat, ainv, diag, targets_in, out,
    targets, lbuf, abuf, dbuf, prod, cum,
    send0, recv0, send1, recv1, sum2a, sum2b, recv2, sum3, recv3,
    tsend0, trecv0, tsend1, trecv1, tsum, trecv2,
    load_sem, relay, s0, r0, s1, r1, s2, r2, s3, r3, top_sem,
):
    yn, zn, slots, share, width = dims
    half = width // 2
    top = top_rows(share)
    row, col = lax.axis_index("row"), lax.axis_index("col")
    y, c = lax.div(row, 2), lax.rem(row, 2)
    z, x = lax.div(col, 2), lax.rem(col, 2)

    def dev(y_, c_, z_, x_):
        return {"row": y_ * 2 + c_, "col": z_ * 2 + x_}

    order = [jnp.where(o < z, o, o + 1) for o in range(zn - 1)] + [z]
    core_peer = dev(y, 1 - c, z, x)
    x_peer = dev(y, c, z, 1 - x)
    y_ids = [lax.rem(y + d, yn) for d in range(1, yn)]
    y_peers = [dev(i, c, z, x) for i in y_ids]
    z_peers = [dev(y, c, zd, x) for zd in order[:-1]]
    z_slots = [jnp.where(z < zd, z, z - 1) for zd in order[:-1]]
    shifts = sorted(range(1, zn), key=lambda d: min(d, zn - d))
    ring = [dev(y, c, lax.rem(z + d, zn), x) for d in (1, zn - 1)]
    near = [core_peer, x_peer] + y_peers + ring

    def local(src, dst, sem):
        return pltpu.make_async_copy(src, dst, sem)

    t_load = local(targets_in, targets, load_sem.at[0])
    t_load.start()
    d_load = local(diag.at[0], dbuf, load_sem.at[1])
    d_load.start()
    for s in range(slots):
        first = s == 0
        local(lhat.at[s], lbuf.at[s], load_sem.at[2 if first else 3]).start()
        local(ainv.at[s], abuf.at[s], load_sem.at[2 if first else 4]).start()

    barrier = pltpu.get_barrier_semaphore()
    for peer in near:
        pl.semaphore_signal(barrier, inc=1, device_id=peer, device_id_type=MESH)

    pair = lbuf.at[pl.ds(0, 2)]
    local(pair, pair, load_sem.at[2]).wait()
    prod[0] = gram_dot(lbuf[0], abuf[0]).reshape(yn, 2, share, width)
    rest = pl.ds(1, slots - 1)
    local(lhat.at[rest], lbuf.at[rest], load_sem.at[3]).wait()
    local(ainv.at[rest], abuf.at[rest], load_sem.at[4]).wait()
    d_load.wait()
    t_load.wait()

    ids = [targets[0, s] for s in range(slots)] + [col]
    count = len(ids)

    def less(k):
        total = jnp.int32(0)
        for t in ids:
            total = total + (t < k).astype(jnp.int32)
        return total

    ranks = []
    for s in range(count):
        rank = jnp.int32(0)
        for r in range(count):
            if r != s:
                before = ids[r] <= ids[s] if r < s else ids[r] < ids[s]
                rank = rank + before.astype(jnp.int32)
        ranks.append(rank)
    sorted_slots = []
    for j in range(count):
        slot = jnp.int32(0)
        for s in range(1, count):
            slot = slot + jnp.where(ranks[s] == j, s, 0)
        sorted_slots.append(slot)

    for s in range(1, slots):
        prod[s] = gram_dot(lbuf[s], abuf[s]).reshape(yn, 2, share, width)
    prod[slots] = -gram_dot(dbuf[...], dbuf[...]).reshape(yn, 2, share, width)

    def prefix(side):
        for yo in range(yn):
            cum[0, yo, side] = jnp.zeros((share, width), jnp.float32)
            total = prod[sorted_slots[0], yo, side]
            cum[1, yo, side] = total
            for j in range(1, count):
                total = total + prod[sorted_slots[j], yo, side]
                cum[j + 1, yo, side] = total

    bounds = {}
    for o in range(zn):
        for xi in range(2):
            k = order[o] * 2 + xi
            bounds[o, xi] = (less(k), less(k + 1))
    top_bounds = {}
    for i, d in enumerate(shifts + [0]):
        for xi in range(2):
            k = lax.rem(z + d, zn) * 2 + xi
            top_bounds[i, xi] = (less(k), less(k + 1))

    def lanes(h):
        return slice(h * half, (h + 1) * half)

    def part(o, h, xi, yo, side):
        begin, end = bounds[o, xi]
        return cum[begin, yo, side, top:, lanes(h)] - cum[end, yo, side, top:, lanes(h)]

    def own_part(o, xi, yo):
        begin = jnp.where(xi == 0, bounds[o, 0][0], bounds[o, 1][0])
        end = jnp.where(xi == 0, bounds[o, 0][1], bounds[o, 1][1])
        return cum[begin, yo, c, top:, lanes(0)] - cum[end, yo, c, top:, lanes(0)]

    def top_part(i, xi, yo, side):
        begin, end = top_bounds[i, xi]
        return cum[begin, yo, side, :top] - cum[end, yo, side, :top]

    def remote(src, dst, send, recv, peer):
        copy = pltpu.make_async_remote_copy(
            src_ref=src, dst_ref=dst, send_sem=send, recv_sem=recv, device_id=peer, device_id_type=MESH
        )
        copy.start()

    def settle(ref, sem):
        local(ref, ref, sem).wait()

    def stage0(o):
        for xi in range(2):
            for yo in range(yn):
                for h in range(2):
                    send0[o, h, xi, yo] = part(o, h, xi, yo, 1 - c)
        if o == 0:
            pl.semaphore_wait(barrier, len(near))
        remote(send0.at[o], recv0.at[o], s0, r0.at[o], core_peer)

    def stage1(o):
        settle(recv0.at[o], r0.at[o])
        for yo in range(yn):
            send1[o, yo] = own_part(o, 1 - x, yo) + recv0[o, 0, 1 - x, yo]
        block = pl.ds(0, yn)
        remote(send1.at[o, block], recv1.at[o, block], s1, r1.at[o], x_peer)
        for i, yo in enumerate(y_ids):
            for xi in range(2):
                send1[o, yn + 2 * i + xi] = part(o, 1, xi, yo, c) + recv0[o, 1, xi, yo]
            block = pl.ds(yn + 2 * i, 2)
            remote(send1.at[o, block], recv1.at[o, block], s1, r1.at[o], y_peers[i])

    def stage2(o):
        settle(recv1.at[o], r1.at[o])
        for yo in range(yn):
            sum2a[o, yo] = own_part(o, x, yo) + recv0[o, 0, x, yo] + recv1[o, yo]
        for i, yo in enumerate(y_ids):
            remote(sum2a.at[o, yo], recv2.at[o, i], s2, r2.at[o], y_peers[i])
        for xi in range(2):
            total = part(o, 1, xi, y, c) + recv0[o, 1, xi, y]
            for i in range(yn - 1):
                total = total + recv1[o, yn + 2 * i + xi]
            sum2b[o, xi] = total
        remote(sum2b.at[o, 1 - x], recv2.at[o, yn - 1], s2, r2.at[o], x_peer)

    def stage3(o):
        settle(recv2.at[o], r2.at[o])
        total = sum2a[o, y]
        for i in range(yn - 1):
            total = total + recv2[o, i]
        sum3[o, 0] = total
        sum3[o, 1] = sum2b[o, x] + recv2[o, yn - 1]
        if o < zn - 1:
            remote(sum3.at[o], recv3.at[z_slots[o]], s3, r3, z_peers[o])

    def top_stage0():
        for i in range(zn):
            for xi in range(2):
                for yo in range(yn):
                    tsend0[i, xi, yo] = top_part(i, xi, yo, 1 - c)
        remote(tsend0, trecv0, top_sem.at[0], top_sem.at[1], core_peer)

    def top_stage1(i):
        for xi in range(2):
            for yo in range(yn):
                tsend1[i, xi, yo] = top_part(i, xi, yo, c) + trecv0[i, xi, yo]
        peer = dev(y, c, lax.rem(z + shifts[i], zn), x)
        remote(tsend1.at[i], trecv1.at[i], top_sem.at[2], top_sem.at[3], peer)

    def top_stage2():
        settle(trecv1, top_sem.at[3])
        for xi in range(2):
            for yo in range(yn):
                total = top_part(zn - 1, xi, yo, c) + trecv0[zn - 1, xi, yo]
                for i in range(zn - 1):
                    total = total + trecv1[i, xi, yo]
                tsum[xi, yo] = total
        for dx in range(2):
            for dy in range(yn):
                if dx or dy:
                    xo, yo = lax.rem(x + dx, 2), lax.rem(y + dy, yn)
                    i = dx * yn + dy - 1
                    remote(tsum.at[xo, yo], trecv2.at[i], top_sem.at[4], top_sem.at[5], dev(yo, c, z, xo))

    def greet(r):
        for peer in ring:
            pl.semaphore_signal(relay.at[r], inc=1, device_id=peer, device_id_type=MESH)

    hops = zn // 2 - 1
    prefix(1 - c)
    stage0(0)
    if hops:
        greet(0)
    if top:
        top_stage0()
    for o in range(1, zn):
        stage0(o)
    prefix(c)
    stage1(0)
    if top:
        settle(trecv0, top_sem.at[1])
        for i in range(2):
            top_stage1(i)
    for o in range(1, zn):
        stage1(o)
    for r in range(hops):
        pl.semaphore_wait(relay.at[r], 2)
        if r < hops - 1:
            greet(r + 1)
    if top:
        for i in range(2, zn - 1):
            top_stage1(i)
    for o in range(zn):
        stage2(o)
    stage3(0)
    if top:
        top_stage2()
    for o in range(1, zn):
        stage3(o)

    settle(recv3, r3)
    for h in range(2):
        total = sum3[zn - 1, h]
        for i in range(zn - 1):
            total = total + recv3[i, h]
        out[0, top:, lanes(h)] = total
    if top:
        settle(trecv2, top_sem.at[5])
        total = tsum[x, y]
        for i in range(2 * yn - 1):
            total = total + trecv2[i]
        out[0, :top] = total
        settle(tsend0, top_sem.at[0])
        settle(tsend1, top_sem.at[2])
        settle(trecv2, top_sem.at[4])
    settle(send0, s0)
    settle(send1, s1)
    settle(recv2, s2)
    settle(recv3, s3)


def on_device(lhat, ainv, diag, targets):
    rows, cols = lax.axis_size("row"), lax.axis_size("col")
    slots, width = lhat.shape[0], lhat.shape[2]
    height = lhat.shape[1]
    yn, zn, share = rows // 2, cols // 2, diag.shape[1]
    half = width // 2
    f32, dma = jnp.float32, pltpu.SemaphoreType.DMA
    top = top_rows(share)
    low = (share - top, half)
    high = (max(top, 8), width)
    scratch = [
        pltpu.SMEM((1, slots), jnp.int32),
        pltpu.VMEM((slots, height, width), f32),
        pltpu.VMEM((slots, height, width), f32),
        pltpu.VMEM((share, width), f32),
        pltpu.VMEM((slots + 1, yn, 2, share, width), f32),
        pltpu.VMEM((slots + 2, yn, 2, share, width), f32),
        pltpu.VMEM((zn, 2, 2, yn) + low, f32),
        pltpu.VMEM((zn, 2, 2, yn) + low, f32),
        pltpu.VMEM((zn, 3 * yn - 2) + low, f32),
        pltpu.VMEM((zn, 3 * yn - 2) + low, f32),
        pltpu.VMEM((zn, yn) + low, f32),
        pltpu.VMEM((zn, 2) + low, f32),
        pltpu.VMEM((zn, yn) + low, f32),
        pltpu.VMEM((zn, 2) + low, f32),
        pltpu.VMEM((zn - 1, 2) + low, f32),
        pltpu.VMEM((zn, 2, yn) + high, f32),
        pltpu.VMEM((zn, 2, yn) + high, f32),
        pltpu.VMEM((zn - 1, 2, yn) + high, f32),
        pltpu.VMEM((zn - 1, 2, yn) + high, f32),
        pltpu.VMEM((2, yn) + high, f32),
        pltpu.VMEM((2 * yn - 1,) + high, f32),
        dma((5,)), pltpu.SemaphoreType.REGULAR((max(zn // 2 - 1, 1),)),
        dma, dma((zn,)), dma, dma((zn,)), dma, dma((zn,)), dma, dma, dma((6,)),
    ]
    return pl.pallas_call(
        functools.partial(kernel, (yn, zn, slots, share, width)),
        out_shape=pltpu.VMEM(diag.shape, f32),
        in_specs=[pl.BlockSpec(memory_space=pltpu.HBM)] * 4,
        out_specs=pl.BlockSpec(memory_space=pltpu.VMEM),
        scratch_shapes=scratch,
        compiler_params=pltpu.CompilerParams(
            collective_id=0, has_side_effects=True, vmem_limit_bytes=60 * 1024 * 1024
        ),
    )(lhat, ainv, diag, targets.T)


def solution(mesh):
    placed = (
        P(("row", "col"), None, None),
        P(("row", "col"), None, None),
        P("col", "row", None),
        P(("row", "col"), None),
    )
    return jax.shard_map(
        on_device, mesh=mesh, in_specs=placed, out_specs=P("col", "row", None), check_vma=False
    )
```

```python
import functools

import jax
import jax.numpy as jnp
from jax import lax
from jax.experimental import pallas as pl
from jax.experimental.pallas import tpu as pltpu
from jax.sharding import PartitionSpec as P

MESH = pl.DeviceIdType.MESH
DN = (((0,), (0,)), ((), ()))
HOLD = 1
T2 = 6


def gram_dot(a, b):
    a_hi = a.astype(jnp.bfloat16)
    a_lo = (a - a_hi.astype(jnp.float32)).astype(jnp.bfloat16)
    b_hi = b.astype(jnp.bfloat16)
    b_lo = (b - b_hi.astype(jnp.float32)).astype(jnp.bfloat16)
    left = jnp.concatenate([a_hi, a_lo, a_hi], axis=0)
    right = jnp.concatenate([b_hi, b_hi, b_lo], axis=0)
    return lax.dot_general(left, right, DN, preferred_element_type=jnp.float32)


def kernel(
    dims,
    lhat, ainv, diag, targets_in, out,
    targets, lbuf, abuf, dbuf, prod, cum,
    send0, recv0, send1, recv1, sum2a, sum2b, recv2, frecv2, sum3, recv3,
    tsend0, trecv0, tsend1, trecv1, tsum, trecv2,
    load_sem, relay, s0, r0, s1, r1, s2, r2, fs2, fr2, s3, r3, top_sem,
):
    yn, zn, slots, share, width = dims
    half = width // 2
    rows = share // 2
    row, col = lax.axis_index("row"), lax.axis_index("col")
    y, c = lax.div(row, 2), lax.rem(row, 2)
    z, x = lax.div(col, 2), lax.rem(col, 2)

    def dev(y_, c_, z_, x_):
        return {"row": y_ * 2 + c_, "col": z_ * 2 + x_}

    def by_plane(values):
        total = jnp.int32(0)
        for q in range(zn):
            total = total + jnp.where(z == q, values[q], 0)
        return total

    far = [[d for d in [0] + list(range(zn - 1, 0, -1)) if d // 2 != q // 2] for q in range(zn)]
    order = [by_plane([far[q][o] for q in range(zn)]) for o in range(zn - 2)] + [z + 1 - 2 * lax.rem(z, 2), z]
    seat = [by_plane([[d for d in far[q] if d % 2 == far[q][o] % 2].index(far[q][o]) for q in range(zn)]) for o in range(zn - 2)]
    kept = zn // 2 - 1
    mine = [[[o for o, d in enumerate(far[q]) if d % 2 == q % 2][e] for q in range(zn)] for e in range(kept)]
    place = [by_plane(mine[e]) for e in range(kept)]
    goal = [by_plane([far[q][mine[e][q]] for q in range(zn)]) for e in range(kept)]
    chunks = [(o, h) for o in range(zn - 2) for h in range(2)] + [(zn - 2, 1), (zn - 1, 1)]
    n_far = 2 * (zn - 2)
    core_peer = dev(y, 1 - c, z, x)
    x_peer = dev(y, c, z, 1 - x)
    y_ids = [lax.rem(y + d, yn) for d in range(1, yn)]
    y_peers = [dev(i, c, z, x) for i in y_ids]
    mate = dev(y, c, z + 1 - 2 * lax.rem(z, 2), x)
    below, above = z > 0, z < zn - 1
    line = [(below, dev(y, c, z - 1, x)), (above, dev(y, c, z + 1, x))]
    n_line = below.astype(jnp.int32) + above.astype(jnp.int32)
    near = [core_peer, x_peer] + y_peers

    def greet(sem):
        for there, peer in line:

            @pl.when(there)
            def _():
                pl.semaphore_signal(sem, inc=1, device_id=peer, device_id_type=MESH)

    def local(src, dst, sem):
        return pltpu.make_async_copy(src, dst, sem)

    t_load = local(targets_in, targets, load_sem.at[0])
    t_load.start()
    d_load = local(diag.at[0], dbuf, load_sem.at[1])
    d_load.start()
    for s in range(slots):
        first = s == 0
        local(lhat.at[s], lbuf.at[s], load_sem.at[2 if first else 3]).start()
        local(ainv.at[s], abuf.at[s], load_sem.at[2 if first else 4]).start()

    barrier = pltpu.get_barrier_semaphore()
    for peer in near:
        pl.semaphore_signal(barrier, inc=1, device_id=peer, device_id_type=MESH)
    greet(barrier)

    pair = lbuf.at[pl.ds(0, 2)]
    local(pair, pair, load_sem.at[2]).wait()
    prod[0] = gram_dot(lbuf[0], abuf[0]).reshape(yn, 2, share, width)
    rest = pl.ds(1, slots - 1)
    local(lhat.at[rest], lbuf.at[rest], load_sem.at[3]).wait()
    local(ainv.at[rest], abuf.at[rest], load_sem.at[4]).wait()
    d_load.wait()
    t_load.wait()

    ids = [targets[0, s] for s in range(slots)] + [col]
    count = len(ids)

    def less(k):
        total = jnp.int32(0)
        for t in ids:
            total = total + (t < k).astype(jnp.int32)
        return total

    ranks = []
    for s in range(count):
        rank = jnp.int32(0)
        for r in range(count):
            if r != s:
                before = ids[r] <= ids[s] if r < s else ids[r] < ids[s]
                rank = rank + before.astype(jnp.int32)
        ranks.append(rank)
    sorted_slots = []
    for j in range(count):
        slot = jnp.int32(0)
        for s in range(1, count):
            slot = slot + jnp.where(ranks[s] == j, s, 0)
        sorted_slots.append(slot)

    for s in range(1, slots):
        prod[s] = gram_dot(lbuf[s], abuf[s]).reshape(yn, 2, share, width)
    prod[slots] = -gram_dot(dbuf[...], dbuf[...]).reshape(yn, 2, share, width)

    def prefix(side):
        for yo in range(yn):
            cum[0, yo, side] = jnp.zeros((share, width), jnp.float32)
            total = prod[sorted_slots[0], yo, side]
            cum[1, yo, side] = total
            for j in range(1, count):
                total = total + prod[sorted_slots[j], yo, side]
                cum[j + 1, yo, side] = total

    bounds = {}
    for o in range(zn):
        for xi in range(2):
            k = order[o] * 2 + xi
            bounds[o, xi] = (less(k), less(k + 1))

    def lanes(h):
        return slice(h * half, (h + 1) * half)

    def span(h):
        return slice(h * rows, (h + 1) * rows)

    def part(i, h, xi, yo, side):
        o, upper = chunks[i]
        begin, end = bounds[o, xi]
        return cum[begin, yo, side, span(upper), lanes(h)] - cum[end, yo, side, span(upper), lanes(h)]

    def own_part(i, xi, yo):
        o, upper = chunks[i]
        begin = jnp.where(xi == 0, bounds[o, 0][0], bounds[o, 1][0])
        end = jnp.where(xi == 0, bounds[o, 0][1], bounds[o, 1][1])
        return cum[begin, yo, c, span(upper), lanes(0)] - cum[end, yo, c, span(upper), lanes(0)]

    def top_part(o, xi, yo, side):
        begin, end = bounds[o + zn - 2, xi]
        return cum[begin, yo, side, span(0)] - cum[end, yo, side, span(0)]

    def remote(src, dst, send, recv, peer):
        copy = pltpu.make_async_remote_copy(
            src_ref=src, dst_ref=dst, send_sem=send, recv_sem=recv, device_id=peer, device_id_type=MESH
        )
        copy.start()

    def settle(ref, sem):
        local(ref, ref, sem).wait()

    def stage0(o):
        for xi in range(2):
            for yo in range(yn):
                for h in range(2):
                    send0[o, h, xi, yo] = part(o, h, xi, yo, 1 - c)
        if o == 0:
            pl.semaphore_wait(barrier, len(near) + n_line)
        remote(send0.at[o], recv0.at[o], s0, r0.at[o], core_peer)

    def stage1(o):
        settle(recv0.at[o], r0.at[o])
        for yo in range(yn):
            send1[o, yo] = own_part(o, 1 - x, yo) + recv0[o, 0, 1 - x, yo]
        block = pl.ds(0, yn)
        remote(send1.at[o, block], recv1.at[o, block], s1, r1.at[o], x_peer)
        for i, yo in enumerate(y_ids):
            for xi in range(2):
                send1[o, yn + 2 * i + xi] = part(o, 1, xi, yo, c) + recv0[o, 1, xi, yo]
            block = pl.ds(yn + 2 * i, 2)
            remote(send1.at[o, block], recv1.at[o, block], s1, r1.at[o], y_peers[i])

    def stage2(o):
        settle(recv1.at[o], r1.at[o])
        for yo in range(yn):
            sum2a[o, yo] = own_part(o, x, yo) + recv0[o, 0, x, yo] + recv1[o, yo]
        plane, upper = chunks[o]
        if o < n_far:
            zc = z - lax.rem(z, 2) + lax.rem(order[plane], 2)
            apart = zc != z
            dest, sem = frecv2.at[seat[plane], upper], fr2.at[seat[plane], upper]
            base = jnp.where(apart, yn, 0)
        else:
            zc, dest, sem, base = z, recv2.at[o - n_far], r2.at[o - n_far], 0
        send_sem = fs2 if o < n_far else s2

        def crossing(copy):
            if o < n_far:

                @pl.when(apart)
                def _():
                    copy()

        for d in range(1, yn):
            yo = lax.rem(y + d, yn)
            remote(sum2a.at[o, yo], dest.at[base + d - 1], send_sem, sem, dev(yo, c, zc, x))
        crossing(lambda: remote(sum2a.at[o, y], dest.at[2 * yn], send_sem, sem, dev(y, c, zc, x)))
        for xi in range(2):
            total = part(o, 1, xi, y, c) + recv0[o, 1, xi, y]
            for i in range(yn - 1):
                total = total + recv1[o, yn + 2 * i + xi]
            sum2b[o, xi] = total
        remote(sum2b.at[o, 1 - x], dest.at[base + yn - 1], send_sem, sem, dev(y, c, zc, 1 - x))
        crossing(lambda: remote(sum2b.at[o, x], dest.at[2 * yn + 1], send_sem, sem, dev(y, c, zc, x)))

    def collect(e, upper):
        settle(frecv2.at[e, upper], fr2.at[e, upper])
        i = place[e] * 2 + upper
        total = sum2a[i, y] + frecv2[e, upper, 2 * yn]
        for d in list(range(yn - 1)) + list(range(yn, 2 * yn - 1)):
            total = total + frecv2[e, upper, d]
        j = 2 * e + upper
        sum3[j, 0] = total
        sum3[j, 1] = sum2b[i, x] + frecv2[e, upper, yn - 1] + frecv2[e, upper, 2 * yn - 1] + frecv2[e, upper, 2 * yn + 1]
        pair, there = lax.div(z, 2), lax.div(goal[e], 2)
        slot = (pair - (pair > there).astype(jnp.int32)) * 2 + upper
        remote(sum3.at[j], recv3.at[slot], s3, r3, dev(y, c, goal[e], x))

    def stage3(i):
        settle(recv2.at[i], r2.at[i])
        o, j = n_far + i, 2 * kept + i
        total = sum2a[o, y]
        for k in range(yn - 1):
            total = total + recv2[i, k]
        sum3[j, 0] = total
        sum3[j, 1] = sum2b[o, x] + recv2[i, yn - 1]
        if i == 0:
            remote(sum3.at[j], recv3.at[2 * kept], s3, r3, mate)

    def top_stage0():
        for i in range(2):
            for xi in range(2):
                for yo in range(yn):
                    tsend0[i, xi, yo] = top_part(i, xi, yo, 1 - c)
        remote(tsend0, trecv0, top_sem.at[0], top_sem.at[1], core_peer)

    def top_stage1():
        settle(trecv0, top_sem.at[1])
        for xi in range(2):
            for yo in range(yn):
                tsend1[xi, yo] = top_part(0, xi, yo, c) + trecv0[0, xi, yo]
        remote(tsend1, trecv1, top_sem.at[2], top_sem.at[3], mate)

    def top_stage2():
        settle(trecv1, top_sem.at[3])
        for xi in range(2):
            for yo in range(yn):
                tsum[xi, yo] = top_part(1, xi, yo, c) + trecv0[1, xi, yo] + trecv1[xi, yo]
        for dx in range(2):
            for dy in range(yn):
                if dx or dy:
                    xo, yo = lax.rem(x + dx, 2), lax.rem(y + dy, yn)
                    i = dx * yn + dy - 1
                    remote(tsum.at[xo, yo], trecv2.at[i], top_sem.at[4], top_sem.at[5], dev(yo, c, z, xo))

    n = len(chunks)
    prefix(1 - c)
    stage0(0)
    if zn > 2:
        greet(relay.at[0])
    stage0(1)
    top_stage0()
    for o in range(2, n):
        stage0(o)
    prefix(c)
    stage1(0)
    stage1(1)
    top_stage1()
    for o in range(2, n - HOLD):
        stage1(o)
    for r in range(zn - 3):
        pl.semaphore_wait(relay.at[r], n_line)
        greet(relay.at[r + 1])
    for o in range(HOLD):
        stage2(o)
        stage1(n - HOLD + o)
    for o in range(HOLD, n):
        if o == T2:
            top_stage2()
        stage2(o)
    if T2 >= n:
        top_stage2()
    if zn > 2:
        pl.semaphore_wait(relay.at[zn - 3], n_line)
    for e in range(kept):
        for upper in range(2):
            collect(e, upper)
    stage3(0)
    stage3(1)

    settle(trecv2, top_sem.at[5])
    total = tsum[x, y]
    for i in range(2 * yn - 1):
        total = total + trecv2[i]
    settle(recv3, r3)
    for h in range(2):
        part0 = total[:, lanes(h)]
        part1 = sum3[2 * kept + 1, h] + recv3[2 * kept, h]
        for i in range(kept):
            part0 = part0 + recv3[2 * i, h]
            part1 = part1 + recv3[2 * i + 1, h]
        out[0, span(0), lanes(h)] = part0
        out[0, span(1), lanes(h)] = part1
    settle(tsend0, top_sem.at[0])
    settle(tsend1, top_sem.at[2])
    settle(trecv2, top_sem.at[4])
    settle(send0, s0)
    settle(send1, s1)
    settle(recv2, s2)
    settle(frecv2, fs2)
    settle(recv3, s3)


def on_device(lhat, ainv, diag, targets):
    rows, cols = lax.axis_size("row"), lax.axis_size("col")
    slots, width = lhat.shape[0], lhat.shape[2]
    height = lhat.shape[1]
    yn, zn, share = rows // 2, cols // 2, diag.shape[1]
    half = width // 2
    f32, dma = jnp.float32, pltpu.SemaphoreType.DMA
    n, kept = 2 * zn - 2, zn // 2 - 1
    low, high = (share // 2, half), (share // 2, width)
    scratch = [
        pltpu.SMEM((1, slots), jnp.int32),
        pltpu.VMEM((slots, height, width), f32),
        pltpu.VMEM((slots, height, width), f32),
        pltpu.VMEM((share, width), f32),
        pltpu.VMEM((slots + 1, yn, 2, share, width), f32),
        pltpu.VMEM((slots + 2, yn, 2, share, width), f32),
        pltpu.VMEM((n, 2, 2, yn) + low, f32),
        pltpu.VMEM((n, 2, 2, yn) + low, f32),
        pltpu.VMEM((n, 3 * yn - 2) + low, f32),
        pltpu.VMEM((n, 3 * yn - 2) + low, f32),
        pltpu.VMEM((n, yn) + low, f32),
        pltpu.VMEM((n, 2) + low, f32),
        pltpu.VMEM((2, yn) + low, f32),
        pltpu.VMEM((kept, 2, 2 * yn + 2) + low, f32),
        pltpu.VMEM((2 * kept + 2, 2) + low, f32),
        pltpu.VMEM((2 * kept + 1, 2) + low, f32),
        pltpu.VMEM((2, 2, yn) + high, f32),
        pltpu.VMEM((2, 2, yn) + high, f32),
        pltpu.VMEM((2, yn) + high, f32),
        pltpu.VMEM((2, yn) + high, f32),
        pltpu.VMEM((2, yn) + high, f32),
        pltpu.VMEM((2 * yn - 1,) + high, f32),
        dma((5,)), pltpu.SemaphoreType.REGULAR((max(zn - 2, 1),)),
        dma, dma((n,)), dma, dma((n,)), dma, dma((2,)), dma, dma((kept, 2)), dma, dma, dma((6,)),
    ]
    return pl.pallas_call(
        functools.partial(kernel, (yn, zn, slots, share, width)),
        out_shape=pltpu.VMEM(diag.shape, f32),
        in_specs=[pl.BlockSpec(memory_space=pltpu.HBM)] * 4,
        out_specs=pl.BlockSpec(memory_space=pltpu.VMEM),
        scratch_shapes=scratch,
        compiler_params=pltpu.CompilerParams(
            collective_id=0, has_side_effects=True, vmem_limit_bytes=60 * 1024 * 1024
        ),
    )(lhat, ainv, diag, targets.T)


def solution(mesh):
    placed = (
        P(("row", "col"), None, None),
        P(("row", "col"), None, None),
        P("col", "row", None),
        P(("row", "col"), None),
    )
    return jax.shard_map(
        on_device, mesh=mesh, in_specs=placed, out_specs=P("col", "row", None), check_vma=False
    )
```

```python
import functools

import jax
import jax.numpy as jnp
from jax import lax
from jax.experimental import pallas as pl
from jax.experimental.pallas import tpu as pltpu
from jax.sharding import PartitionSpec as P

MESH = pl.DeviceIdType.MESH
DN = (((0,), (0,)), ((), ()))
HOLD = 1
T2 = 6


def gram_dot(a, b):
    a_hi = a.astype(jnp.bfloat16)
    a_lo = (a - a_hi.astype(jnp.float32)).astype(jnp.bfloat16)
    b_hi = b.astype(jnp.bfloat16)
    b_lo = (b - b_hi.astype(jnp.float32)).astype(jnp.bfloat16)
    left = jnp.concatenate([a_hi, a_lo, a_hi], axis=0)
    right = jnp.concatenate([b_hi, b_hi, b_lo], axis=0)
    return lax.dot_general(left, right, DN, preferred_element_type=jnp.float32)


def dot_groups(slots):
    cuts = sorted({min(slots, cut) for cut in (0, 1, 4)} | {slots})
    return list(zip(cuts, cuts[1:]))


def kernel(
    dims,
    lhat, ainv, diag, targets_in, out,
    targets, lbuf, abuf, dbuf, prod, cum,
    send0, recv0, send1, recv1, sum2a, sum2b, recv2, frecv2, sum3, recv3,
    tsend0, trecv0, tsend1, trecv1, tsum, trecv2,
    load_sem, relay, cross, s0, r0, s1, r1, s2, r2, fs2, fr2, s3, r3, top_sem,
):
    yn, zn, slots, share, width = dims
    half = width // 2
    rows = share // 2
    row, col = lax.axis_index("row"), lax.axis_index("col")
    y, c = lax.div(row, 2), lax.rem(row, 2)
    z, x = lax.div(col, 2), lax.rem(col, 2)

    def dev(y_, c_, z_, x_):
        return {"row": y_ * 2 + c_, "col": z_ * 2 + x_}

    def by_plane(values):
        total = jnp.int32(0)
        for q in range(zn):
            total = total + jnp.where(z == q, values[q], 0)
        return total

    far = [[d for d in [0] + list(range(zn - 1, 0, -1)) if d // 2 != q // 2] for q in range(zn)]
    order = [by_plane([far[q][o] for q in range(zn)]) for o in range(zn - 2)] + [z + 1 - 2 * lax.rem(z, 2), z]
    seat = [by_plane([[d for d in far[q] if d % 2 == far[q][o] % 2].index(far[q][o]) for q in range(zn)]) for o in range(zn - 2)]
    kept = zn // 2 - 1
    mine = [[[o for o, d in enumerate(far[q]) if d % 2 == q % 2][e] for q in range(zn)] for e in range(kept)]
    place = [by_plane(mine[e]) for e in range(kept)]
    goal = [by_plane([far[q][mine[e][q]] for q in range(zn)]) for e in range(kept)]
    chunks = [(o, h) for o in range(zn - 2) for h in range(2)] + [(zn - 2, 1), (zn - 1, 1)]
    n_far = 2 * (zn - 2)
    core_peer = dev(y, 1 - c, z, x)
    x_peer = dev(y, c, z, 1 - x)
    y_ids = [lax.rem(y + d, yn) for d in range(1, yn)]
    y_peers = [dev(i, c, z, x) for i in y_ids]
    mate = dev(y, c, z + 1 - 2 * lax.rem(z, 2), x)
    below, above = z > 0, z < zn - 1
    line = [(below, dev(y, c, z - 1, x)), (above, dev(y, c, z + 1, x))]
    n_line = below.astype(jnp.int32) + above.astype(jnp.int32)
    near = [core_peer, x_peer] + y_peers

    def greet(sem):
        for there, peer in line:

            @pl.when(there)
            def _():
                pl.semaphore_signal(sem, inc=1, device_id=peer, device_id_type=MESH)

    def local(src, dst, sem):
        return pltpu.make_async_copy(src, dst, sem)

    t_load = local(targets_in, targets, load_sem.at[0])
    t_load.start()
    d_load = local(diag.at[0], dbuf, load_sem.at[1])
    d_load.start()
    groups = dot_groups(slots)
    for g, (first, last) in enumerate(groups):
        for s in range(first, last):
            local(lhat.at[s], lbuf.at[s], load_sem.at[2 + 2 * g]).start()
            local(ainv.at[s], abuf.at[s], load_sem.at[3 + 2 * g]).start()

    barrier = pltpu.get_barrier_semaphore()
    for peer in near:
        pl.semaphore_signal(barrier, inc=1, device_id=peer, device_id_type=MESH)
    greet(barrier)

    def loaded(g):
        first, last = groups[g]
        part = pl.ds(first, last - first)
        local(lhat.at[part], lbuf.at[part], load_sem.at[2 + 2 * g]).wait()
        local(ainv.at[part], abuf.at[part], load_sem.at[3 + 2 * g]).wait()

    def multiply(g):
        for s in range(*groups[g]):
            prod[s] = gram_dot(lbuf[s], abuf[s]).reshape(yn, 2, share, width)

    for g in range(len(groups) - 1):
        loaded(g)
        multiply(g)
    loaded(len(groups) - 1)
    d_load.wait()
    t_load.wait()

    ids = [targets[0, s] for s in range(slots)] + [col]
    count = len(ids)

    def less(k):
        total = jnp.int32(0)
        for t in ids:
            total = total + (t < k).astype(jnp.int32)
        return total

    ranks = []
    for s in range(count):
        rank = jnp.int32(0)
        for r in range(count):
            if r != s:
                before = ids[r] <= ids[s] if r < s else ids[r] < ids[s]
                rank = rank + before.astype(jnp.int32)
        ranks.append(rank)
    sorted_slots = []
    for j in range(count):
        slot = jnp.int32(0)
        for s in range(1, count):
            slot = slot + jnp.where(ranks[s] == j, s, 0)
        sorted_slots.append(slot)

    multiply(len(groups) - 1)
    prod[slots] = -gram_dot(dbuf[...], dbuf[...]).reshape(yn, 2, share, width)

    def prefix(side):
        for yo in range(yn):
            cum[0, yo, side] = jnp.zeros((share, width), jnp.float32)
            total = prod[sorted_slots[0], yo, side]
            cum[1, yo, side] = total
            for j in range(1, count):
                total = total + prod[sorted_slots[j], yo, side]
                cum[j + 1, yo, side] = total

    bounds = {}
    for o in range(zn):
        for xi in range(2):
            k = order[o] * 2 + xi
            bounds[o, xi] = (less(k), less(k + 1))

    def lanes(h):
        return slice(h * half, (h + 1) * half)

    def span(h):
        return slice(h * rows, (h + 1) * rows)

    def side_of(i):
        return 1 - c if i < n_far else c

    def part(i, h, xi, yo, side):
        o, upper = chunks[i]
        begin, end = bounds[o, xi]
        return cum[begin, yo, side, span(upper), lanes(h)] - cum[end, yo, side, span(upper), lanes(h)]

    def own_part(i, xi, yo):
        o, upper = chunks[i]
        begin = jnp.where(xi == 0, bounds[o, 0][0], bounds[o, 1][0])
        end = jnp.where(xi == 0, bounds[o, 0][1], bounds[o, 1][1])
        side = side_of(i)
        return cum[begin, yo, side, span(upper), lanes(0)] - cum[end, yo, side, span(upper), lanes(0)]

    def top_part(o, xi, yo, side):
        begin, end = bounds[o + zn - 2, xi]
        return cum[begin, yo, side, span(0)] - cum[end, yo, side, span(0)]

    def remote(src, dst, send, recv, peer):
        copy = pltpu.make_async_remote_copy(
            src_ref=src, dst_ref=dst, send_sem=send, recv_sem=recv, device_id=peer, device_id_type=MESH
        )
        copy.start()

    def settle(ref, sem):
        local(ref, ref, sem).wait()

    def stage0(o):
        for xi in range(2):
            for yo in range(yn):
                for h in range(2):
                    send0[o, h, xi, yo] = part(o, h, xi, yo, 1 - side_of(o))
        if o == 0:
            pl.semaphore_wait(barrier, len(near) + n_line)
        remote(send0.at[o], recv0.at[o], s0, r0.at[o], core_peer)

    def stage1(o):
        settle(recv0.at[o], r0.at[o])
        for yo in range(yn):
            send1[o, yo] = own_part(o, 1 - x, yo) + recv0[o, 0, 1 - x, yo]
        block = pl.ds(0, yn)
        remote(send1.at[o, block], recv1.at[o, block], s1, r1.at[o], x_peer)
        for i, yo in enumerate(y_ids):
            for xi in range(2):
                send1[o, yn + 2 * i + xi] = part(o, 1, xi, yo, side_of(o)) + recv0[o, 1, xi, yo]
            block = pl.ds(yn + 2 * i, 2)
            remote(send1.at[o, block], recv1.at[o, block], s1, r1.at[o], y_peers[i])

    def stage2(o):
        settle(recv1.at[o], r1.at[o])
        for yo in range(yn):
            sum2a[o, yo] = own_part(o, x, yo) + recv0[o, 0, x, yo] + recv1[o, yo]
        plane, upper = chunks[o]
        if o < n_far:
            zc = z - lax.rem(z, 2) + lax.rem(order[plane], 2)
            apart = zc != z
            dest, sem = frecv2.at[seat[plane], upper], fr2.at[seat[plane], upper]
            base = jnp.where(apart, yn, 0)
        else:
            zc, dest, sem, base = z, recv2.at[o - n_far], r2.at[o - n_far], 0
        send_sem = fs2 if o < n_far else s2

        def crossing(copy):
            if o < n_far:

                @pl.when(apart)
                def _():
                    copy()

        for d in range(1, yn):
            yo = lax.rem(y + d, yn)
            remote(sum2a.at[o, yo], dest.at[base + d - 1], send_sem, sem, dev(yo, c, zc, x))
        crossing(lambda: remote(sum2a.at[o, y], dest.at[2 * yn], send_sem, sem, dev(y, c, zc, x)))
        for xi in range(2):
            total = part(o, 1, xi, y, side_of(o)) + recv0[o, 1, xi, y]
            for i in range(yn - 1):
                total = total + recv1[o, yn + 2 * i + xi]
            sum2b[o, xi] = total
        remote(sum2b.at[o, 1 - x], dest.at[base + yn - 1], send_sem, sem, dev(y, c, zc, 1 - x))
        crossing(lambda: remote(sum2b.at[o, x], dest.at[2 * yn + 1], send_sem, sem, dev(y, c, zc, x)))

    def collect(e, upper):
        settle(frecv2.at[e, upper], fr2.at[e, upper])
        i = place[e] * 2 + upper
        total = sum2a[i, y] + frecv2[e, upper, 2 * yn]
        for d in list(range(yn - 1)) + list(range(yn, 2 * yn - 1)):
            total = total + frecv2[e, upper, d]
        j = 2 * e + upper
        sum3[j, 0] = total
        sum3[j, 1] = sum2b[i, x] + frecv2[e, upper, yn - 1] + frecv2[e, upper, 2 * yn - 1] + frecv2[e, upper, 2 * yn + 1]
        pair, there = lax.div(z, 2), lax.div(goal[e], 2)
        slot = (pair - (pair > there).astype(jnp.int32)) * 2 + upper
        remote(sum3.at[j], recv3.at[slot], s3, r3, dev(y, 1 - c, goal[e], x))

    def stage3(i):
        settle(recv2.at[i], r2.at[i])
        o, j = n_far + i, 2 * kept + i
        total = sum2a[o, y]
        for k in range(yn - 1):
            total = total + recv2[i, k]
        sum3[j, 0] = total
        sum3[j, 1] = sum2b[o, x] + recv2[i, yn - 1]
        if i == 0:
            remote(sum3.at[j], recv3.at[2 * kept], s3, r3, mate)

    def top_stage0():
        for i in range(2):
            for xi in range(2):
                for yo in range(yn):
                    tsend0[i, xi, yo] = top_part(i, xi, yo, 1 - c)
        remote(tsend0, trecv0, top_sem.at[0], top_sem.at[1], core_peer)

    def top_stage1():
        settle(trecv0, top_sem.at[1])
        for xi in range(2):
            for yo in range(yn):
                tsend1[xi, yo] = top_part(0, xi, yo, c) + trecv0[0, xi, yo]
        remote(tsend1, trecv1, top_sem.at[2], top_sem.at[3], mate)

    def top_stage2():
        settle(trecv1, top_sem.at[3])
        for xi in range(2):
            for yo in range(yn):
                tsum[xi, yo] = top_part(1, xi, yo, c) + trecv0[1, xi, yo] + trecv1[xi, yo]
        for dx in range(2):
            for dy in range(yn):
                if dx or dy:
                    xo, yo = lax.rem(x + dx, 2), lax.rem(y + dy, yn)
                    i = dx * yn + dy - 1
                    remote(tsum.at[xo, yo], trecv2.at[i], top_sem.at[4], top_sem.at[5], dev(yo, c, z, xo))

    n = len(chunks)
    prefix(c)
    stage0(0)
    if zn > 2:
        greet(relay.at[0])
    stage0(1)
    prefix(1 - c)
    top_stage0()
    for o in range(2, n):
        stage0(o)
    stage1(0)
    stage1(1)
    top_stage1()
    for o in range(2, n - HOLD):
        stage1(o)
    for r in range(zn - 3):
        pl.semaphore_wait(relay.at[r], n_line)
        greet(relay.at[r + 1])
    for o in range(HOLD):
        stage2(o)
        stage1(n - HOLD + o)
    for o in range(HOLD, n):
        if o == T2:
            top_stage2()
        stage2(o)
    if T2 >= n:
        top_stage2()
    if zn > 2:
        pl.semaphore_wait(relay.at[zn - 3], n_line)
        pl.semaphore_signal(cross, inc=1, device_id=core_peer, device_id_type=MESH)
        pl.semaphore_wait(cross, 1)
    for e in range(kept):
        for upper in range(2):
            collect(e, upper)
    stage3(0)
    stage3(1)

    settle(trecv2, top_sem.at[5])
    total = tsum[x, y]
    for i in range(2 * yn - 1):
        total = total + trecv2[i]
    settle(recv3, r3)
    for h in range(2):
        part0 = total[:, lanes(h)]
        part1 = sum3[2 * kept + 1, h] + recv3[2 * kept, h]
        for i in range(kept):
            part0 = part0 + recv3[2 * i, h]
            part1 = part1 + recv3[2 * i + 1, h]
        out[0, span(0), lanes(h)] = part0
        out[0, span(1), lanes(h)] = part1
    settle(tsend0, top_sem.at[0])
    settle(tsend1, top_sem.at[2])
    settle(trecv2, top_sem.at[4])
    settle(send0, s0)
    settle(send1, s1)
    settle(recv2, s2)
    settle(frecv2, fs2)
    settle(recv3, s3)


def on_device(lhat, ainv, diag, targets):
    rows, cols = lax.axis_size("row"), lax.axis_size("col")
    slots, width = lhat.shape[0], lhat.shape[2]
    height = lhat.shape[1]
    yn, zn, share = rows // 2, cols // 2, diag.shape[1]
    half = width // 2
    f32, dma = jnp.float32, pltpu.SemaphoreType.DMA
    n, kept = 2 * zn - 2, zn // 2 - 1
    low, high = (share // 2, half), (share // 2, width)
    scratch = [
        pltpu.SMEM((1, slots), jnp.int32),
        pltpu.VMEM((slots, height, width), f32),
        pltpu.VMEM((slots, height, width), f32),
        pltpu.VMEM((share, width), f32),
        pltpu.VMEM((slots + 1, yn, 2, share, width), f32),
        pltpu.VMEM((slots + 2, yn, 2, share, width), f32),
        pltpu.VMEM((n, 2, 2, yn) + low, f32),
        pltpu.VMEM((n, 2, 2, yn) + low, f32),
        pltpu.VMEM((n, 3 * yn - 2) + low, f32),
        pltpu.VMEM((n, 3 * yn - 2) + low, f32),
        pltpu.VMEM((n, yn) + low, f32),
        pltpu.VMEM((n, 2) + low, f32),
        pltpu.VMEM((2, yn) + low, f32),
        pltpu.VMEM((kept, 2, 2 * yn + 2) + low, f32),
        pltpu.VMEM((2 * kept + 2, 2) + low, f32),
        pltpu.VMEM((2 * kept + 1, 2) + low, f32),
        pltpu.VMEM((2, 2, yn) + high, f32),
        pltpu.VMEM((2, 2, yn) + high, f32),
        pltpu.VMEM((2, yn) + high, f32),
        pltpu.VMEM((2, yn) + high, f32),
        pltpu.VMEM((2, yn) + high, f32),
        pltpu.VMEM((2 * yn - 1,) + high, f32),
        dma((2 + 2 * len(dot_groups(slots)),)), pltpu.SemaphoreType.REGULAR((max(zn - 2, 1),)),
        pltpu.SemaphoreType.REGULAR, dma, dma((n,)), dma, dma((n,)), dma, dma((2,)), dma, dma((kept, 2)), dma, dma, dma((6,)),
    ]
    return pl.pallas_call(
        functools.partial(kernel, (yn, zn, slots, share, width)),
        out_shape=pltpu.VMEM(diag.shape, f32),
        in_specs=[pl.BlockSpec(memory_space=pltpu.HBM)] * 4,
        out_specs=pl.BlockSpec(memory_space=pltpu.VMEM),
        scratch_shapes=scratch,
        compiler_params=pltpu.CompilerParams(
            collective_id=0, has_side_effects=True, vmem_limit_bytes=60 * 1024 * 1024
        ),
    )(lhat, ainv, diag, targets.T)


def solution(mesh):
    placed = (
        P(("row", "col"), None, None),
        P(("row", "col"), None, None),
        P("col", "row", None),
        P(("row", "col"), None),
    )
    return jax.shard_map(
        on_device, mesh=mesh, in_specs=placed, out_specs=P("col", "row", None), check_vma=False
    )
```

```python
import functools

import jax
import jax.numpy as jnp
from jax import lax
from jax.experimental import pallas as pl
from jax.experimental.pallas import tpu as pltpu
from jax.sharding import PartitionSpec as P

MESH = pl.DeviceIdType.MESH
DN = (((0,), (0,)), ((), ()))
HOLD = 1
T2 = 6


def gram_dot(a, b):
    a_hi = a.astype(jnp.bfloat16)
    a_lo = (a - a_hi.astype(jnp.float32)).astype(jnp.bfloat16)
    b_hi = b.astype(jnp.bfloat16)
    b_lo = (b - b_hi.astype(jnp.float32)).astype(jnp.bfloat16)
    left = jnp.concatenate([a_hi, a_lo, a_hi], axis=0)
    right = jnp.concatenate([b_hi, b_hi, b_lo], axis=0)
    return lax.dot_general(left, right, DN, preferred_element_type=jnp.float32)


def dot_groups(slots):
    cuts = sorted({min(slots, cut) for cut in (0, 1, 4)} | {slots})
    return list(zip(cuts, cuts[1:]))


def kernel(
    dims,
    lhat, ainv, diag, targets_in, out,
    targets, lbuf, abuf, dbuf, prod, cum,
    send0, recv0, send1, recv1, sum2a, sum2b, recv2, frecv2, sum3, recv3,
    tsend0, trecv0, tsend1, trecv1, tsum, trecv2,
    load_sem, relay, cross, s0, r0, s1, r1, s2, r2, fs2, fr2, s3, r3, top_sem,
):
    yn, zn, slots, share, width = dims
    half = width // 2
    rows = share // 2
    row, col = lax.axis_index("row"), lax.axis_index("col")
    y, c = lax.div(row, 2), lax.rem(row, 2)
    z, x = lax.div(col, 2), lax.rem(col, 2)

    def dev(y_, c_, z_, x_):
        return {"row": y_ * 2 + c_, "col": z_ * 2 + x_}

    def by_plane(values):
        total = jnp.int32(0)
        for q in range(zn):
            total = total + jnp.where(z == q, values[q], 0)
        return total

    far = [[d for d in [0] + list(range(zn - 1, 0, -1)) if d // 2 != q // 2] for q in range(zn)]
    order = [by_plane([far[q][o] for q in range(zn)]) for o in range(zn - 2)] + [z + 1 - 2 * lax.rem(z, 2), z]
    mirrored = z >= zn // 2
    kept_half = jnp.where(mirrored, 1 - lax.rem(z, 2), lax.rem(z, 2))
    kept = zn // 2 - 1
    chunks = [(o, h) for o in range(zn - 2) for h in range(2)] + [(zn - 2, 1), (zn - 1, 1)]
    n_far = 2 * (zn - 2)
    core_peer = dev(y, 1 - c, z, x)
    x_peer = dev(y, c, z, 1 - x)
    y_ids = [lax.rem(y + d, yn) for d in range(1, yn)]
    y_peers = [dev(i, c, z, x) for i in y_ids]
    mate = dev(y, c, z + 1 - 2 * lax.rem(z, 2), x)
    twin = dev(y, 1 - c, z + 1 - 2 * lax.rem(z, 2), x)
    below, above = z > 0, z < zn - 1
    line = [(below, dev(y, c, z - 1, x)), (above, dev(y, c, z + 1, x))]
    n_line = below.astype(jnp.int32) + above.astype(jnp.int32)
    near = [core_peer, x_peer] + y_peers

    def greet(sem):
        for there, peer in line:

            @pl.when(there)
            def _():
                pl.semaphore_signal(sem, inc=1, device_id=peer, device_id_type=MESH)

    def local(src, dst, sem):
        return pltpu.make_async_copy(src, dst, sem)

    t_load = local(targets_in, targets, load_sem.at[0])
    t_load.start()
    d_load = local(diag.at[0], dbuf, load_sem.at[1])
    d_load.start()
    groups = dot_groups(slots)
    for g, (first, last) in enumerate(groups):
        for s in range(first, last):
            local(lhat.at[s], lbuf.at[s], load_sem.at[2 + 2 * g]).start()
            local(ainv.at[s], abuf.at[s], load_sem.at[3 + 2 * g]).start()

    barrier = pltpu.get_barrier_semaphore()
    for peer in near:
        pl.semaphore_signal(barrier, inc=1, device_id=peer, device_id_type=MESH)
    greet(barrier)

    def loaded(g):
        first, last = groups[g]
        part = pl.ds(first, last - first)
        local(lhat.at[part], lbuf.at[part], load_sem.at[2 + 2 * g]).wait()
        local(ainv.at[part], abuf.at[part], load_sem.at[3 + 2 * g]).wait()

    def multiply(g):
        for s in range(*groups[g]):
            prod[s] = gram_dot(lbuf[s], abuf[s]).reshape(yn, 2, share, width)

    for g in range(len(groups) - 1):
        loaded(g)
        multiply(g)
    loaded(len(groups) - 1)
    d_load.wait()
    t_load.wait()

    ids = [targets[0, s] for s in range(slots)] + [col]
    count = len(ids)

    def less(k):
        total = jnp.int32(0)
        for t in ids:
            total = total + (t < k).astype(jnp.int32)
        return total

    ranks = []
    for s in range(count):
        rank = jnp.int32(0)
        for r in range(count):
            if r != s:
                before = ids[r] <= ids[s] if r < s else ids[r] < ids[s]
                rank = rank + before.astype(jnp.int32)
        ranks.append(rank)
    sorted_slots = []
    for j in range(count):
        slot = jnp.int32(0)
        for s in range(1, count):
            slot = slot + jnp.where(ranks[s] == j, s, 0)
        sorted_slots.append(slot)

    multiply(len(groups) - 1)
    prod[slots] = -gram_dot(dbuf[...], dbuf[...]).reshape(yn, 2, share, width)

    def prefix(side):
        for yo in range(yn):
            cum[0, yo, side] = jnp.zeros((share, width), jnp.float32)
            total = prod[sorted_slots[0], yo, side]
            cum[1, yo, side] = total
            for j in range(1, count):
                total = total + prod[sorted_slots[j], yo, side]
                cum[j + 1, yo, side] = total

    bounds = {}
    for o in range(zn):
        for xi in range(2):
            k = order[o] * 2 + xi
            bounds[o, xi] = (less(k), less(k + 1))

    def lanes(h):
        return slice(h * half, (h + 1) * half)

    def span(h):
        return slice(h * rows, (h + 1) * rows)

    def side_of(i):
        return 1 - c if i <= n_far else c

    def part(i, h, xi, yo, side):
        o, upper = chunks[i]
        begin, end = bounds[o, xi]
        return cum[begin, yo, side, span(upper), lanes(h)] - cum[end, yo, side, span(upper), lanes(h)]

    def own_part(i, xi, yo):
        o, upper = chunks[i]
        begin = jnp.where(xi == 0, bounds[o, 0][0], bounds[o, 1][0])
        end = jnp.where(xi == 0, bounds[o, 0][1], bounds[o, 1][1])
        side = side_of(i)
        return cum[begin, yo, side, span(upper), lanes(0)] - cum[end, yo, side, span(upper), lanes(0)]

    def top_part(o, xi, yo, side):
        begin, end = bounds[o + zn - 2, xi]
        return cum[begin, yo, side, span(0)] - cum[end, yo, side, span(0)]

    def remote(src, dst, send, recv, peer):
        copy = pltpu.make_async_remote_copy(
            src_ref=src, dst_ref=dst, send_sem=send, recv_sem=recv, device_id=peer, device_id_type=MESH
        )
        copy.start()

    def settle(ref, sem):
        local(ref, ref, sem).wait()

    def stage0(o):
        for xi in range(2):
            for yo in range(yn):
                for h in range(2):
                    send0[o, h, xi, yo] = part(o, h, xi, yo, 1 - side_of(o))
        if o == 0:
            pl.semaphore_wait(barrier, len(near) + n_line)
        remote(send0.at[o], recv0.at[o], s0, r0.at[o], core_peer)

    def stage1(o):
        settle(recv0.at[o], r0.at[o])
        for yo in range(yn):
            send1[o, yo] = own_part(o, 1 - x, yo) + recv0[o, 0, 1 - x, yo]
        block = pl.ds(0, yn)
        remote(send1.at[o, block], recv1.at[o, block], s1, r1.at[o], x_peer)
        for i, yo in enumerate(y_ids):
            for xi in range(2):
                send1[o, yn + 2 * i + xi] = part(o, 1, xi, yo, side_of(o)) + recv0[o, 1, xi, yo]
            block = pl.ds(yn + 2 * i, 2)
            remote(send1.at[o, block], recv1.at[o, block], s1, r1.at[o], y_peers[i])

    def stage2(o):
        settle(recv1.at[o], r1.at[o])
        for yo in range(yn):
            sum2a[o, yo] = own_part(o, x, yo) + recv0[o, 0, x, yo] + recv1[o, yo]
        plane, upper = chunks[o]
        if o < n_far:
            zc = z - lax.rem(z, 2) + jnp.where(mirrored, 1 - upper, upper)
            apart = zc != z
            dest, sem = frecv2.at[plane], fr2.at[plane]
            base = jnp.where(apart, yn, 0)
        else:
            zc, dest, sem, base = z, recv2.at[o - n_far], r2.at[o - n_far], 0
        send_sem = fs2 if o < n_far else s2

        def crossing(copy):
            if o < n_far:

                @pl.when(apart)
                def _():
                    copy()

        for d in range(1, yn):
            yo = lax.rem(y + d, yn)
            remote(sum2a.at[o, yo], dest.at[base + d - 1], send_sem, sem, dev(yo, c, zc, x))
        crossing(lambda: remote(sum2a.at[o, y], dest.at[2 * yn], send_sem, sem, dev(y, c, zc, x)))
        for xi in range(2):
            total = part(o, 1, xi, y, side_of(o)) + recv0[o, 1, xi, y]
            for i in range(yn - 1):
                total = total + recv1[o, yn + 2 * i + xi]
            sum2b[o, xi] = total
        remote(sum2b.at[o, 1 - x], dest.at[base + yn - 1], send_sem, sem, dev(y, c, zc, 1 - x))
        crossing(lambda: remote(sum2b.at[o, x], dest.at[2 * yn + 1], send_sem, sem, dev(y, c, zc, x)))

    def collect(e):
        settle(frecv2.at[e], fr2.at[e])
        i = e * 2 + kept_half
        total = sum2a[i, y] + frecv2[e, 2 * yn]
        for d in list(range(yn - 1)) + list(range(yn, 2 * yn - 1)):
            total = total + frecv2[e, d]
        sum3[e, 0] = total
        sum3[e, 1] = sum2b[i, x] + frecv2[e, yn - 1] + frecv2[e, 2 * yn - 1] + frecv2[e, 2 * yn + 1]
        pair, there = lax.div(z, 2), lax.div(order[e], 2)
        slot = (pair - (pair > there).astype(jnp.int32)) * 2 + kept_half
        remote(sum3.at[e], recv3.at[slot], s3, r3, dev(y, 1 - c, order[e], x))

    def stage3(i):
        settle(recv2.at[i], r2.at[i])
        o, j = n_far + i, 2 * kept + i
        total = sum2a[o, y]
        for k in range(yn - 1):
            total = total + recv2[i, k]
        sum3[j, 0] = total
        sum3[j, 1] = sum2b[o, x] + recv2[i, yn - 1]
        if i == 0:
            remote(sum3.at[j], recv3.at[2 * kept], s3, r3, twin)

    def top_stage0():
        for i in range(2):
            for xi in range(2):
                for yo in range(yn):
                    tsend0[i, xi, yo] = top_part(i, xi, yo, 1 - c)
        remote(tsend0, trecv0, top_sem.at[0], top_sem.at[1], core_peer)

    def top_stage1():
        settle(trecv0, top_sem.at[1])
        for xi in range(2):
            for yo in range(yn):
                tsend1[xi, yo] = top_part(0, xi, yo, c) + trecv0[0, xi, yo]
        remote(tsend1, trecv1, top_sem.at[2], top_sem.at[3], mate)

    def top_stage2():
        settle(trecv1, top_sem.at[3])
        for xi in range(2):
            for yo in range(yn):
                tsum[xi, yo] = top_part(1, xi, yo, c) + trecv0[1, xi, yo] + trecv1[xi, yo]
        for dx in range(2):
            for dy in range(yn):
                if dx or dy:
                    xo, yo = lax.rem(x + dx, 2), lax.rem(y + dy, yn)
                    i = dx * yn + dy - 1
                    remote(tsum.at[xo, yo], trecv2.at[i], top_sem.at[4], top_sem.at[5], dev(yo, c, z, xo))

    n = len(chunks)
    prefix(c)
    stage0(0)
    if zn > 2:
        greet(relay.at[0])
    stage0(1)
    prefix(1 - c)
    top_stage0()
    for o in range(2, n):
        stage0(o)
    stage1(0)
    stage1(1)
    top_stage1()
    for o in range(2, n - HOLD):
        stage1(o)
    for r in range(zn - 3):
        pl.semaphore_wait(relay.at[r], n_line)
        greet(relay.at[r + 1])
    for o in range(HOLD):
        stage2(o)
        stage1(n - HOLD + o)
    for o in range(HOLD, n):
        if o == 2:
            pl.semaphore_wait(relay.at[zn - 3], n_line)
            pl.semaphore_signal(cross, inc=1, device_id=core_peer, device_id_type=MESH)
        if o == n - 1:
            pl.semaphore_wait(cross, 1)
            collect(0)
        stage2(o)
    top_stage2()
    for e in range(1, zn - 2):
        collect(e)
    stage3(0)
    stage3(1)

    settle(trecv2, top_sem.at[5])
    total = tsum[x, y]
    for i in range(2 * yn - 1):
        total = total + trecv2[i]
    settle(recv3, r3)
    for h in range(2):
        part0 = total[:, lanes(h)]
        part1 = sum3[2 * kept + 1, h] + recv3[2 * kept, h]
        for i in range(kept):
            part0 = part0 + recv3[2 * i, h]
            part1 = part1 + recv3[2 * i + 1, h]
        out[0, span(0), lanes(h)] = part0
        out[0, span(1), lanes(h)] = part1
    settle(tsend0, top_sem.at[0])
    settle(tsend1, top_sem.at[2])
    settle(trecv2, top_sem.at[4])
    settle(send0, s0)
    settle(send1, s1)
    settle(recv2, s2)
    settle(frecv2, fs2)
    settle(recv3, s3)


def on_device(lhat, ainv, diag, targets):
    rows, cols = lax.axis_size("row"), lax.axis_size("col")
    slots, width = lhat.shape[0], lhat.shape[2]
    height = lhat.shape[1]
    yn, zn, share = rows // 2, cols // 2, diag.shape[1]
    half = width // 2
    f32, dma = jnp.float32, pltpu.SemaphoreType.DMA
    n, kept = 2 * zn - 2, zn // 2 - 1
    low, high = (share // 2, half), (share // 2, width)
    scratch = [
        pltpu.SMEM((1, slots), jnp.int32),
        pltpu.VMEM((slots, height, width), f32),
        pltpu.VMEM((slots, height, width), f32),
        pltpu.VMEM((share, width), f32),
        pltpu.VMEM((slots + 1, yn, 2, share, width), f32),
        pltpu.VMEM((slots + 2, yn, 2, share, width), f32),
        pltpu.VMEM((n, 2, 2, yn) + low, f32),
        pltpu.VMEM((n, 2, 2, yn) + low, f32),
        pltpu.VMEM((n, 3 * yn - 2) + low, f32),
        pltpu.VMEM((n, 3 * yn - 2) + low, f32),
        pltpu.VMEM((n, yn) + low, f32),
        pltpu.VMEM((n, 2) + low, f32),
        pltpu.VMEM((2, yn) + low, f32),
        pltpu.VMEM((zn - 2, 2 * yn + 2) + low, f32),
        pltpu.VMEM((2 * kept + 2, 2) + low, f32),
        pltpu.VMEM((2 * kept + 1, 2) + low, f32),
        pltpu.VMEM((2, 2, yn) + high, f32),
        pltpu.VMEM((2, 2, yn) + high, f32),
        pltpu.VMEM((2, yn) + high, f32),
        pltpu.VMEM((2, yn) + high, f32),
        pltpu.VMEM((2, yn) + high, f32),
        pltpu.VMEM((2 * yn - 1,) + high, f32),
        dma((2 + 2 * len(dot_groups(slots)),)), pltpu.SemaphoreType.REGULAR((max(zn - 2, 1),)),
        pltpu.SemaphoreType.REGULAR, dma, dma((n,)), dma, dma((n,)), dma, dma((2,)), dma, dma((zn - 2,)), dma, dma, dma((6,)),
    ]
    return pl.pallas_call(
        functools.partial(kernel, (yn, zn, slots, share, width)),
        out_shape=pltpu.VMEM(diag.shape, f32),
        in_specs=[pl.BlockSpec(memory_space=pltpu.HBM)] * 4,
        out_specs=pl.BlockSpec(memory_space=pltpu.VMEM),
        scratch_shapes=scratch,
        compiler_params=pltpu.CompilerParams(
            collective_id=0, has_side_effects=True, vmem_limit_bytes=60 * 1024 * 1024
        ),
    )(lhat, ainv, diag, targets.T)


def solution(mesh):
    placed = (
        P(("row", "col"), None, None),
        P(("row", "col"), None, None),
        P("col", "row", None),
        P(("row", "col"), None),
    )
    return jax.shard_map(
        on_device, mesh=mesh, in_specs=placed, out_specs=P("col", "row", None), check_vma=False
    )
```

```python
import functools

import jax
import jax.numpy as jnp
from jax import lax
from jax.experimental import pallas as pl
from jax.experimental.pallas import tpu as pltpu
from jax.sharding import PartitionSpec as P

MESH = pl.DeviceIdType.MESH
DN = (((0,), (0,)), ((), ()))
HOLD = 1
T2 = 6


def gram_dot(a, b):
    a_hi = a.astype(jnp.bfloat16)
    a_lo = (a - a_hi.astype(jnp.float32)).astype(jnp.bfloat16)
    b_hi = b.astype(jnp.bfloat16)
    b_lo = (b - b_hi.astype(jnp.float32)).astype(jnp.bfloat16)
    left = jnp.concatenate([a_hi, a_lo, a_hi], axis=0)
    right = jnp.concatenate([b_hi, b_hi, b_lo], axis=0)
    return lax.dot_general(left, right, DN, preferred_element_type=jnp.float32)


def dot_groups(slots):
    cuts = sorted({min(slots, cut) for cut in (0, 1, 4)} | {slots})
    return list(zip(cuts, cuts[1:]))


def kernel(
    dims,
    lhat, ainv, diag, targets_in, out,
    targets, lbuf, abuf, dbuf, prod, cum,
    send0, recv0, send1, recv1, sum2a, sum2b, recv2, frecv2, sum3, recv3,
    tsend0, trecv0, tsend1, trecv1, tsum, trecv2,
    load_sem, relay, cross, s0, r0, s1, r1, s2, r2, fs2, fr2, s3, r3, top_sem,
):
    yn, zn, slots, share, width = dims
    half = width // 2
    rows = share // 2
    row, col = lax.axis_index("row"), lax.axis_index("col")
    y, c = lax.div(row, 2), lax.rem(row, 2)
    z, x = lax.div(col, 2), lax.rem(col, 2)

    def dev(y_, c_, z_, x_):
        return {"row": y_ * 2 + c_, "col": z_ * 2 + x_}

    def by_plane(values):
        total = jnp.int32(0)
        for q in range(zn):
            total = total + jnp.where(z == q, values[q], 0)
        return total

    far = [[d for d in [0] + list(range(zn - 1, 0, -1)) if d // 2 != q // 2] for q in range(zn)]
    order = [by_plane([far[q][o] for q in range(zn)]) for o in range(zn - 2)] + [z + 1 - 2 * lax.rem(z, 2), z]
    mirrored = z >= zn // 2
    kept_half = jnp.where(mirrored, 1 - lax.rem(z, 2), lax.rem(z, 2))
    kept = zn // 2 - 1
    chunks = [(o, h) for o in range(zn - 2) for h in range(2)] + [(zn - 2, 1), (zn - 1, 1)]
    n_far = 2 * (zn - 2)
    core_peer = dev(y, 1 - c, z, x)
    x_peer = dev(y, c, z, 1 - x)
    y_ids = [lax.rem(y + d, yn) for d in range(1, yn)]
    y_peers = [dev(i, c, z, x) for i in y_ids]
    mate = dev(y, c, z + 1 - 2 * lax.rem(z, 2), x)
    twin = dev(y, 1 - c, z + 1 - 2 * lax.rem(z, 2), x)
    below, above = z > 0, z < zn - 1
    line = [(below, dev(y, c, z - 1, x)), (above, dev(y, c, z + 1, x))]
    n_line = below.astype(jnp.int32) + above.astype(jnp.int32)
    near = [core_peer, x_peer] + y_peers

    def greet(sem):
        for there, peer in line:

            @pl.when(there)
            def _():
                pl.semaphore_signal(sem, inc=1, device_id=peer, device_id_type=MESH)

    def local(src, dst, sem):
        return pltpu.make_async_copy(src, dst, sem)

    t_load = local(targets_in, targets, load_sem.at[0])
    t_load.start()
    d_load = local(diag.at[0], dbuf, load_sem.at[1])
    d_load.start()
    groups = dot_groups(slots)
    for g, (first, last) in enumerate(groups):
        for s in range(first, last):
            local(lhat.at[s], lbuf.at[s], load_sem.at[2 + 2 * g]).start()
            local(ainv.at[s], abuf.at[s], load_sem.at[3 + 2 * g]).start()

    barrier = pltpu.get_barrier_semaphore()
    for peer in near:
        pl.semaphore_signal(barrier, inc=1, device_id=peer, device_id_type=MESH)
    greet(barrier)

    def loaded(g):
        first, last = groups[g]
        part = pl.ds(first, last - first)
        local(lhat.at[part], lbuf.at[part], load_sem.at[2 + 2 * g]).wait()
        local(ainv.at[part], abuf.at[part], load_sem.at[3 + 2 * g]).wait()

    def multiply(g):
        for s in range(*groups[g]):
            prod[s] = gram_dot(lbuf[s], abuf[s]).reshape(yn, 2, share, width)

    loaded(0)
    d_load.wait()
    t_load.wait()

    ids = [targets[0, s] for s in range(slots)] + [col]
    count = len(ids)

    def less(k):
        total = jnp.int32(0)
        for t in ids:
            total = total + (t < k).astype(jnp.int32)
        return total

    ranks = []
    for s in range(count):
        rank = jnp.int32(0)
        for r in range(count):
            if r != s:
                before = ids[r] <= ids[s] if r < s else ids[r] < ids[s]
                rank = rank + before.astype(jnp.int32)
        ranks.append(rank)
    sorted_slots = []
    for j in range(count):
        slot = jnp.int32(0)
        for s in range(1, count):
            slot = slot + jnp.where(ranks[s] == j, s, 0)
        sorted_slots.append(slot)

    multiply(0)
    prod[slots] = -gram_dot(dbuf[...], dbuf[...]).reshape(yn, 2, share, width)
    for g in range(1, len(groups) - 1):
        loaded(g)
        multiply(g)
    loaded(len(groups) - 1)
    multiply(len(groups) - 1)

    def prefix(side):
        for yo in range(yn):
            cum[0, yo, side] = jnp.zeros((share, width), jnp.float32)
            total = prod[sorted_slots[0], yo, side]
            cum[1, yo, side] = total
            for j in range(1, count):
                total = total + prod[sorted_slots[j], yo, side]
                cum[j + 1, yo, side] = total

    bounds = {}
    for o in range(zn):
        for xi in range(2):
            k = order[o] * 2 + xi
            bounds[o, xi] = (less(k), less(k + 1))

    def lanes(h):
        return slice(h * half, (h + 1) * half)

    def span(h):
        return slice(h * rows, (h + 1) * rows)

    def side_of(i):
        return 1 - c if i <= n_far else c

    def part(i, h, xi, yo, side):
        o, upper = chunks[i]
        begin, end = bounds[o, xi]
        return cum[begin, yo, side, span(upper), lanes(h)] - cum[end, yo, side, span(upper), lanes(h)]

    def own_part(i, xi, yo):
        o, upper = chunks[i]
        begin = jnp.where(xi == 0, bounds[o, 0][0], bounds[o, 1][0])
        end = jnp.where(xi == 0, bounds[o, 0][1], bounds[o, 1][1])
        side = side_of(i)
        return cum[begin, yo, side, span(upper), lanes(0)] - cum[end, yo, side, span(upper), lanes(0)]

    def top_part(o, xi, yo, side):
        begin, end = bounds[o + zn - 2, xi]
        return cum[begin, yo, side, span(0)] - cum[end, yo, side, span(0)]

    def remote(src, dst, send, recv, peer):
        copy = pltpu.make_async_remote_copy(
            src_ref=src, dst_ref=dst, send_sem=send, recv_sem=recv, device_id=peer, device_id_type=MESH
        )
        copy.start()

    def settle(ref, sem):
        local(ref, ref, sem).wait()

    def stage0(o):
        for xi in range(2):
            for yo in range(yn):
                for h in range(2):
                    send0[o, h, xi, yo] = part(o, h, xi, yo, 1 - side_of(o))
        if o == 0:
            pl.semaphore_wait(barrier, len(near) + n_line)
        remote(send0.at[o], recv0.at[o], s0, r0.at[o], core_peer)

    def stage1(o):
        settle(recv0.at[o], r0.at[o])
        for yo in range(yn):
            send1[o, yo] = own_part(o, 1 - x, yo) + recv0[o, 0, 1 - x, yo]
        block = pl.ds(0, yn)
        remote(send1.at[o, block], recv1.at[o, block], s1, r1.at[o], x_peer)
        for i, yo in enumerate(y_ids):
            for xi in range(2):
                send1[o, yn + 2 * i + xi] = part(o, 1, xi, yo, side_of(o)) + recv0[o, 1, xi, yo]
            block = pl.ds(yn + 2 * i, 2)
            remote(send1.at[o, block], recv1.at[o, block], s1, r1.at[o], y_peers[i])

    def stage2(o):
        settle(recv1.at[o], r1.at[o])
        for yo in range(yn):
            sum2a[o, yo] = own_part(o, x, yo) + recv0[o, 0, x, yo] + recv1[o, yo]
        plane, upper = chunks[o]
        if o < n_far:
            zc = z - lax.rem(z, 2) + jnp.where(mirrored, 1 - upper, upper)
            apart = zc != z
            dest, sem = frecv2.at[plane], fr2.at[plane]
            base = jnp.where(apart, yn, 0)
        else:
            zc, dest, sem, base = z, recv2.at[o - n_far], r2.at[o - n_far], 0
        send_sem = fs2 if o < n_far else s2

        def crossing(copy):
            if o < n_far:

                @pl.when(apart)
                def _():
                    copy()

        for d in range(1, yn):
            yo = lax.rem(y + d, yn)
            remote(sum2a.at[o, yo], dest.at[base + d - 1], send_sem, sem, dev(yo, c, zc, x))
        crossing(lambda: remote(sum2a.at[o, y], dest.at[2 * yn], send_sem, sem, dev(y, c, zc, x)))
        for xi in range(2):
            total = part(o, 1, xi, y, side_of(o)) + recv0[o, 1, xi, y]
            for i in range(yn - 1):
                total = total + recv1[o, yn + 2 * i + xi]
            sum2b[o, xi] = total
        remote(sum2b.at[o, 1 - x], dest.at[base + yn - 1], send_sem, sem, dev(y, c, zc, 1 - x))
        crossing(lambda: remote(sum2b.at[o, x], dest.at[2 * yn + 1], send_sem, sem, dev(y, c, zc, x)))

    def collect(e):
        settle(frecv2.at[e], fr2.at[e])
        i = e * 2 + kept_half
        total = sum2a[i, y] + frecv2[e, 2 * yn]
        for d in list(range(yn - 1)) + list(range(yn, 2 * yn - 1)):
            total = total + frecv2[e, d]
        sum3[e, 0] = total
        sum3[e, 1] = sum2b[i, x] + frecv2[e, yn - 1] + frecv2[e, 2 * yn - 1] + frecv2[e, 2 * yn + 1]
        pair, there = lax.div(z, 2), lax.div(order[e], 2)
        slot = (pair - (pair > there).astype(jnp.int32)) * 2 + kept_half
        remote(sum3.at[e], recv3.at[slot], s3, r3, dev(y, 1 - c, order[e], x))

    def stage3(i):
        settle(recv2.at[i], r2.at[i])
        o, j = n_far + i, 2 * kept + i
        total = sum2a[o, y]
        for k in range(yn - 1):
            total = total + recv2[i, k]
        sum3[j, 0] = total
        sum3[j, 1] = sum2b[o, x] + recv2[i, yn - 1]
        if i == 0:
            remote(sum3.at[j], recv3.at[2 * kept], s3, r3, twin)

    def top_stage0():
        for i in range(2):
            for xi in range(2):
                for yo in range(yn):
                    tsend0[i, xi, yo] = top_part(i, xi, yo, 1 - c)
        remote(tsend0, trecv0, top_sem.at[0], top_sem.at[1], core_peer)

    def top_stage1():
        settle(trecv0, top_sem.at[1])
        for xi in range(2):
            for yo in range(yn):
                tsend1[xi, yo] = top_part(0, xi, yo, c) + trecv0[0, xi, yo]
        remote(tsend1, trecv1, top_sem.at[2], top_sem.at[3], mate)

    def top_stage2():
        settle(trecv1, top_sem.at[3])
        for xi in range(2):
            for yo in range(yn):
                tsum[xi, yo] = top_part(1, xi, yo, c) + trecv0[1, xi, yo] + trecv1[xi, yo]
        for dx in range(2):
            for dy in range(yn):
                if dx or dy:
                    xo, yo = lax.rem(x + dx, 2), lax.rem(y + dy, yn)
                    i = dx * yn + dy - 1
                    remote(tsum.at[xo, yo], trecv2.at[i], top_sem.at[4], top_sem.at[5], dev(yo, c, z, xo))

    n = len(chunks)
    prefix(c)
    stage0(0)
    if zn > 2:
        greet(relay.at[0])
    stage0(1)
    prefix(1 - c)
    top_stage0()
    for o in range(2, n):
        stage0(o)
    stage1(0)
    stage1(1)
    top_stage1()
    for o in range(2, n - HOLD):
        stage1(o)
    for r in range(zn - 3):
        pl.semaphore_wait(relay.at[r], n_line)
        greet(relay.at[r + 1])
    for o in range(HOLD):
        stage2(o)
        stage1(n - HOLD + o)
    for o in range(HOLD, n):
        if o == 2:
            pl.semaphore_wait(relay.at[zn - 3], n_line)
            pl.semaphore_signal(cross, inc=1, device_id=core_peer, device_id_type=MESH)
        if o == n - 1:
            pl.semaphore_wait(cross, 1)

            @pl.when(mirrored)
            def _():
                collect(0)

        stage2(o)
    top_stage2()

    @pl.when(jnp.logical_not(mirrored))
    def _():
        collect(0)

    @pl.when(mirrored)
    def _():
        for e in range(1, zn - 2):
            collect(e)

    stage3(0)

    @pl.when(jnp.logical_not(mirrored))
    def _():
        for e in range(1, zn - 2):
            collect(e)

    stage3(1)

    settle(trecv2, top_sem.at[5])
    total = tsum[x, y]
    for i in range(2 * yn - 1):
        total = total + trecv2[i]
    settle(recv3, r3)
    for h in range(2):
        part0 = total[:, lanes(h)]
        part1 = sum3[2 * kept + 1, h] + recv3[2 * kept, h]
        for i in range(kept):
            part0 = part0 + recv3[2 * i, h]
            part1 = part1 + recv3[2 * i + 1, h]
        out[0, span(0), lanes(h)] = part0
        out[0, span(1), lanes(h)] = part1
    settle(tsend0, top_sem.at[0])
    settle(tsend1, top_sem.at[2])
    settle(trecv2, top_sem.at[4])
    settle(send0, s0)
    settle(send1, s1)
    settle(recv2, s2)
    settle(frecv2, fs2)
    settle(recv3, s3)


def on_device(lhat, ainv, diag, targets):
    rows, cols = lax.axis_size("row"), lax.axis_size("col")
    slots, width = lhat.shape[0], lhat.shape[2]
    height = lhat.shape[1]
    yn, zn, share = rows // 2, cols // 2, diag.shape[1]
    half = width // 2
    f32, dma = jnp.float32, pltpu.SemaphoreType.DMA
    n, kept = 2 * zn - 2, zn // 2 - 1
    low, high = (share // 2, half), (share // 2, width)
    scratch = [
        pltpu.SMEM((1, slots), jnp.int32),
        pltpu.VMEM((slots, height, width), f32),
        pltpu.VMEM((slots, height, width), f32),
        pltpu.VMEM((share, width), f32),
        pltpu.VMEM((slots + 1, yn, 2, share, width), f32),
        pltpu.VMEM((slots + 2, yn, 2, share, width), f32),
        pltpu.VMEM((n, 2, 2, yn) + low, f32),
        pltpu.VMEM((n, 2, 2, yn) + low, f32),
        pltpu.VMEM((n, 3 * yn - 2) + low, f32),
        pltpu.VMEM((n, 3 * yn - 2) + low, f32),
        pltpu.VMEM((n, yn) + low, f32),
        pltpu.VMEM((n, 2) + low, f32),
        pltpu.VMEM((2, yn) + low, f32),
        pltpu.VMEM((zn - 2, 2 * yn + 2) + low, f32),
        pltpu.VMEM((2 * kept + 2, 2) + low, f32),
        pltpu.VMEM((2 * kept + 1, 2) + low, f32),
        pltpu.VMEM((2, 2, yn) + high, f32),
        pltpu.VMEM((2, 2, yn) + high, f32),
        pltpu.VMEM((2, yn) + high, f32),
        pltpu.VMEM((2, yn) + high, f32),
        pltpu.VMEM((2, yn) + high, f32),
        pltpu.VMEM((2 * yn - 1,) + high, f32),
        dma((2 + 2 * len(dot_groups(slots)),)), pltpu.SemaphoreType.REGULAR((max(zn - 2, 1),)),
        pltpu.SemaphoreType.REGULAR, dma, dma((n,)), dma, dma((n,)), dma, dma((2,)), dma, dma((zn - 2,)), dma, dma, dma((6,)),
    ]
    return pl.pallas_call(
        functools.partial(kernel, (yn, zn, slots, share, width)),
        out_shape=pltpu.VMEM(diag.shape, f32),
        in_specs=[pl.BlockSpec(memory_space=pltpu.HBM)] * 4,
        out_specs=pl.BlockSpec(memory_space=pltpu.VMEM),
        scratch_shapes=scratch,
        compiler_params=pltpu.CompilerParams(
            collective_id=0, has_side_effects=True, vmem_limit_bytes=60 * 1024 * 1024
        ),
    )(lhat, ainv, diag, targets.T)


def solution(mesh):
    placed = (
        P(("row", "col"), None, None),
        P(("row", "col"), None, None),
        P("col", "row", None),
        P(("row", "col"), None),
    )
    return jax.shard_map(
        on_device, mesh=mesh, in_specs=placed, out_specs=P("col", "row", None), check_vma=False
    )
```

```python
import functools

import jax
import jax.numpy as jnp
from jax import lax
from jax.experimental import pallas as pl
from jax.experimental.pallas import tpu as pltpu
from jax.sharding import PartitionSpec as P

MESH = pl.DeviceIdType.MESH
DN = (((0,), (0,)), ((), ()))
HOLD = 1
T2 = 6


def gram_dot(a, b):
    a_hi = a.astype(jnp.bfloat16)
    a_lo = (a - a_hi.astype(jnp.float32)).astype(jnp.bfloat16)
    b_hi = b.astype(jnp.bfloat16)
    b_lo = (b - b_hi.astype(jnp.float32)).astype(jnp.bfloat16)
    left = jnp.concatenate([a_hi, a_lo, a_hi], axis=0)
    right = jnp.concatenate([b_hi, b_hi, b_lo], axis=0)
    return lax.dot_general(left, right, DN, preferred_element_type=jnp.float32)


def dot_groups(slots):
    cuts = sorted({min(slots, cut) for cut in (0, 1, 4)} | {slots})
    return list(zip(cuts, cuts[1:]))


def kernel(
    dims,
    lhat, ainv, diag, targets_in, out,
    targets, lbuf, abuf, dbuf, prod, cum,
    send0, recv0, send1, recv1, sum2a, sum2b, recv2, frecv2, sum3, recv3,
    tsend0, trecv0, tsend1, trecv1, tsum, trecv2,
    load_sem, relay, cross, s0, r0, s1, r1, s2, r2, fs2, fr2, s3, r3, top_sem,
):
    yn, zn, slots, share, width = dims
    half = width // 2
    rows = share // 2
    row, col = lax.axis_index("row"), lax.axis_index("col")
    y, c = lax.div(row, 2), lax.rem(row, 2)
    z, x = lax.div(col, 2), lax.rem(col, 2)

    def dev(y_, c_, z_, x_):
        return {"row": y_ * 2 + c_, "col": z_ * 2 + x_}

    def by_plane(values):
        total = jnp.int32(0)
        for q in range(zn):
            total = total + jnp.where(z == q, values[q], 0)
        return total

    far = [[d for d in [0] + list(range(zn - 1, 0, -1)) if d // 2 != q // 2] for q in range(zn)]
    order = [by_plane([far[q][o] for q in range(zn)]) for o in range(zn - 2)] + [z + 1 - 2 * lax.rem(z, 2), z]
    mirrored = z >= zn // 2
    kept_half = jnp.where(mirrored, 1 - lax.rem(z, 2), lax.rem(z, 2))
    kept = zn // 2 - 1
    chunks = [(o, h) for o in range(zn - 2) for h in range(2)] + [(zn - 2, 1), (zn - 1, 1)]
    n_far = 2 * (zn - 2)
    core_peer = dev(y, 1 - c, z, x)
    x_peer = dev(y, c, z, 1 - x)
    y_ids = [lax.rem(y + d, yn) for d in range(1, yn)]
    y_peers = [dev(i, c, z, x) for i in y_ids]
    mate = dev(y, c, z + 1 - 2 * lax.rem(z, 2), x)
    twin = dev(y, 1 - c, z + 1 - 2 * lax.rem(z, 2), x)
    below, above = z > 0, z < zn - 1
    line = [(below, dev(y, c, z - 1, x)), (above, dev(y, c, z + 1, x))]
    n_line = below.astype(jnp.int32) + above.astype(jnp.int32)
    near = [core_peer, x_peer] + y_peers

    def greet(sem):
        for there, peer in line:

            @pl.when(there)
            def _():
                pl.semaphore_signal(sem, inc=1, device_id=peer, device_id_type=MESH)

    def local(src, dst, sem):
        return pltpu.make_async_copy(src, dst, sem)

    t_load = local(targets_in, targets, load_sem.at[0])
    t_load.start()
    d_load = local(diag.at[0], dbuf, load_sem.at[1])
    d_load.start()
    groups = dot_groups(slots)
    for g, (first, last) in enumerate(groups):
        for s in range(first, last):
            local(lhat.at[s], lbuf.at[s], load_sem.at[2 + g]).start()
            local(ainv.at[s], abuf.at[s], load_sem.at[2 + g]).start()

    barrier = pltpu.get_barrier_semaphore()
    for peer in near:
        pl.semaphore_signal(barrier, inc=1, device_id=peer, device_id_type=MESH)
    greet(barrier)

    def loaded(g):
        first, last = groups[g]
        both = lbuf.at[pl.ds(0, 2 * (last - first))]
        local(both, both, load_sem.at[2 + g]).wait()

    def multiply(g):
        for s in range(*groups[g]):
            prod[s] = gram_dot(lbuf[s], abuf[s]).reshape(yn, 2, share, width)

    loaded(0)
    d_load.wait()
    t_load.wait()

    ids = [targets[0, s] for s in range(slots)] + [col]
    count = len(ids)

    def less(k):
        total = jnp.int32(0)
        for t in ids:
            total = total + (t < k).astype(jnp.int32)
        return total

    ranks = []
    for s in range(count):
        rank = jnp.int32(0)
        for r in range(count):
            if r != s:
                before = ids[r] <= ids[s] if r < s else ids[r] < ids[s]
                rank = rank + before.astype(jnp.int32)
        ranks.append(rank)
    sorted_slots = []
    for j in range(count):
        slot = jnp.int32(0)
        for s in range(1, count):
            slot = slot + jnp.where(ranks[s] == j, s, 0)
        sorted_slots.append(slot)

    multiply(0)
    prod[slots] = -gram_dot(dbuf[...], dbuf[...]).reshape(yn, 2, share, width)
    for g in range(1, len(groups) - 1):
        loaded(g)
        multiply(g)
    loaded(len(groups) - 1)
    multiply(len(groups) - 1)

    def prefix(side):
        for yo in range(yn):
            cum[0, yo, side] = jnp.zeros((share, width), jnp.float32)
            total = prod[sorted_slots[0], yo, side]
            cum[1, yo, side] = total
            for j in range(1, count):
                total = total + prod[sorted_slots[j], yo, side]
                cum[j + 1, yo, side] = total

    bounds = {}
    for o in range(zn):
        for xi in range(2):
            k = order[o] * 2 + xi
            bounds[o, xi] = (less(k), less(k + 1))

    def lanes(h):
        return slice(h * half, (h + 1) * half)

    def span(h):
        return slice(h * rows, (h + 1) * rows)

    def side_of(i):
        return 1 - c if i <= n_far else c

    def part(i, h, xi, yo, side):
        o, upper = chunks[i]
        begin, end = bounds[o, xi]
        return cum[begin, yo, side, span(upper), lanes(h)] - cum[end, yo, side, span(upper), lanes(h)]

    def own_part(i, xi, yo):
        o, upper = chunks[i]
        begin = jnp.where(xi == 0, bounds[o, 0][0], bounds[o, 1][0])
        end = jnp.where(xi == 0, bounds[o, 0][1], bounds[o, 1][1])
        side = side_of(i)
        return cum[begin, yo, side, span(upper), lanes(0)] - cum[end, yo, side, span(upper), lanes(0)]

    def top_part(o, xi, yo, side):
        begin, end = bounds[o + zn - 2, xi]
        return cum[begin, yo, side, span(0)] - cum[end, yo, side, span(0)]

    def remote(src, dst, send, recv, peer):
        copy = pltpu.make_async_remote_copy(
            src_ref=src, dst_ref=dst, send_sem=send, recv_sem=recv, device_id=peer, device_id_type=MESH
        )
        copy.start()

    def settle(ref, sem):
        local(ref, ref, sem).wait()

    def stage0(o):
        for xi in range(2):
            for yo in range(yn):
                for h in range(2):
                    send0[o, h, xi, yo] = part(o, h, xi, yo, 1 - side_of(o))
        if o == 0:
            pl.semaphore_wait(barrier, len(near) + n_line)
        remote(send0.at[o], recv0.at[o], s0, r0.at[o], core_peer)

    def stage1(o):
        settle(recv0.at[o], r0.at[o])
        for yo in range(yn):
            send1[o, yo] = own_part(o, 1 - x, yo) + recv0[o, 0, 1 - x, yo]
        block = pl.ds(0, yn)
        remote(send1.at[o, block], recv1.at[o, block], s1, r1.at[o], x_peer)
        for i, yo in enumerate(y_ids):
            for xi in range(2):
                send1[o, yn + 2 * i + xi] = part(o, 1, xi, yo, side_of(o)) + recv0[o, 1, xi, yo]
            block = pl.ds(yn + 2 * i, 2)
            remote(send1.at[o, block], recv1.at[o, block], s1, r1.at[o], y_peers[i])

    def stage2(o):
        settle(recv1.at[o], r1.at[o])
        for yo in range(yn):
            sum2a[o, yo] = own_part(o, x, yo) + recv0[o, 0, x, yo] + recv1[o, yo]
        plane, upper = chunks[o]
        if o < n_far:
            zc = z - lax.rem(z, 2) + jnp.where(mirrored, 1 - upper, upper)
            apart = zc != z
            dest, sem = frecv2.at[plane], fr2.at[plane]
            base = jnp.where(apart, yn, 0)
        else:
            zc, dest, sem, base = z, recv2.at[o - n_far], r2.at[o - n_far], 0
        send_sem = fs2 if o < n_far else s2

        def crossing(copy):
            if o < n_far:

                @pl.when(apart)
                def _():
                    copy()

        for d in range(1, yn):
            yo = lax.rem(y + d, yn)
            remote(sum2a.at[o, yo], dest.at[base + d - 1], send_sem, sem, dev(yo, c, zc, x))
        crossing(lambda: remote(sum2a.at[o, y], dest.at[2 * yn], send_sem, sem, dev(y, c, zc, x)))
        for xi in range(2):
            total = part(o, 1, xi, y, side_of(o)) + recv0[o, 1, xi, y]
            for i in range(yn - 1):
                total = total + recv1[o, yn + 2 * i + xi]
            sum2b[o, xi] = total
        remote(sum2b.at[o, 1 - x], dest.at[base + yn - 1], send_sem, sem, dev(y, c, zc, 1 - x))
        crossing(lambda: remote(sum2b.at[o, x], dest.at[2 * yn + 1], send_sem, sem, dev(y, c, zc, x)))

    def collect(e):
        settle(frecv2.at[e], fr2.at[e])
        i = e * 2 + kept_half
        total = sum2a[i, y] + frecv2[e, 2 * yn]
        for d in list(range(yn - 1)) + list(range(yn, 2 * yn - 1)):
            total = total + frecv2[e, d]
        sum3[e, 0] = total
        sum3[e, 1] = sum2b[i, x] + frecv2[e, yn - 1] + frecv2[e, 2 * yn - 1] + frecv2[e, 2 * yn + 1]
        pair, there = lax.div(z, 2), lax.div(order[e], 2)
        slot = (pair - (pair > there).astype(jnp.int32)) * 2 + kept_half
        remote(sum3.at[e], recv3.at[slot], s3, r3, dev(y, 1 - c, order[e], x))

    def stage3(i):
        settle(recv2.at[i], r2.at[i])
        o, j = n_far + i, 2 * kept + i
        total = sum2a[o, y]
        for k in range(yn - 1):
            total = total + recv2[i, k]
        sum3[j, 0] = total
        sum3[j, 1] = sum2b[o, x] + recv2[i, yn - 1]
        if i == 0:
            remote(sum3.at[j], recv3.at[2 * kept], s3, r3, twin)

    def top_stage0():
        for i in range(2):
            for xi in range(2):
                for yo in range(yn):
                    tsend0[i, xi, yo] = top_part(i, xi, yo, 1 - c)
        remote(tsend0, trecv0, top_sem.at[0], top_sem.at[1], core_peer)

    def top_stage1():
        settle(trecv0, top_sem.at[1])
        for xi in range(2):
            for yo in range(yn):
                tsend1[xi, yo] = top_part(0, xi, yo, c) + trecv0[0, xi, yo]
        remote(tsend1, trecv1, top_sem.at[2], top_sem.at[3], mate)

    def top_stage2():
        settle(trecv1, top_sem.at[3])
        for xi in range(2):
            for yo in range(yn):
                tsum[xi, yo] = top_part(1, xi, yo, c) + trecv0[1, xi, yo] + trecv1[xi, yo]
        for dx in range(2):
            for dy in range(yn):
                if dx or dy:
                    xo, yo = lax.rem(x + dx, 2), lax.rem(y + dy, yn)
                    i = dx * yn + dy - 1
                    remote(tsum.at[xo, yo], trecv2.at[i], top_sem.at[4], top_sem.at[5], dev(yo, c, z, xo))

    n = len(chunks)
    prefix(c)
    stage0(0)
    if zn > 2:
        greet(relay.at[0])
    stage0(1)
    prefix(1 - c)
    top_stage0()
    for o in range(2, n):
        stage0(o)
    stage1(0)
    stage1(1)
    top_stage1()
    for o in range(2, n - HOLD):
        stage1(o)
    for r in range(zn - 3):
        pl.semaphore_wait(relay.at[r], n_line)
        greet(relay.at[r + 1])
    for o in range(HOLD):
        stage2(o)
        stage1(n - HOLD + o)
    for o in range(HOLD, n):
        if o == 2:
            pl.semaphore_wait(relay.at[zn - 3], n_line)
            pl.semaphore_signal(cross, inc=1, device_id=core_peer, device_id_type=MESH)
        if o == n - 1:
            pl.semaphore_wait(cross, 1)

            @pl.when(mirrored)
            def _():
                collect(0)

        stage2(o)
    top_stage2()

    @pl.when(jnp.logical_not(mirrored))
    def _():
        collect(0)

    @pl.when(mirrored)
    def _():
        for e in range(1, zn - 2):
            collect(e)

    stage3(0)

    @pl.when(jnp.logical_not(mirrored))
    def _():
        for e in range(1, zn - 2):
            collect(e)

    stage3(1)

    settle(trecv2, top_sem.at[5])
    total = tsum[x, y]
    for i in range(2 * yn - 1):
        total = total + trecv2[i]
    settle(recv3, r3)
    for h in range(2):
        part0 = total[:, lanes(h)]
        part1 = sum3[2 * kept + 1, h] + recv3[2 * kept, h]
        for i in range(kept):
            part0 = part0 + recv3[2 * i, h]
            part1 = part1 + recv3[2 * i + 1, h]
        out[0, span(0), lanes(h)] = part0
        out[0, span(1), lanes(h)] = part1
    settle(tsend0, top_sem.at[0])
    settle(tsend1, top_sem.at[2])
    settle(trecv2, top_sem.at[4])
    settle(send0, s0)
    settle(send1, s1)
    settle(recv2, s2)
    settle(frecv2, fs2)
    settle(recv3, s3)


def on_device(lhat, ainv, diag, targets):
    rows, cols = lax.axis_size("row"), lax.axis_size("col")
    slots, width = lhat.shape[0], lhat.shape[2]
    height = lhat.shape[1]
    yn, zn, share = rows // 2, cols // 2, diag.shape[1]
    half = width // 2
    f32, dma = jnp.float32, pltpu.SemaphoreType.DMA
    n, kept = 2 * zn - 2, zn // 2 - 1
    low, high = (share // 2, half), (share // 2, width)
    scratch = [
        pltpu.SMEM((1, slots), jnp.int32),
        pltpu.VMEM((slots, height, width), f32),
        pltpu.VMEM((slots, height, width), f32),
        pltpu.VMEM((share, width), f32),
        pltpu.VMEM((slots + 1, yn, 2, share, width), f32),
        pltpu.VMEM((slots + 2, yn, 2, share, width), f32),
        pltpu.VMEM((n, 2, 2, yn) + low, f32),
        pltpu.VMEM((n, 2, 2, yn) + low, f32),
        pltpu.VMEM((n, 3 * yn - 2) + low, f32),
        pltpu.VMEM((n, 3 * yn - 2) + low, f32),
        pltpu.VMEM((n, yn) + low, f32),
        pltpu.VMEM((n, 2) + low, f32),
        pltpu.VMEM((2, yn) + low, f32),
        pltpu.VMEM((zn - 2, 2 * yn + 2) + low, f32),
        pltpu.VMEM((2 * kept + 2, 2) + low, f32),
        pltpu.VMEM((2 * kept + 1, 2) + low, f32),
        pltpu.VMEM((2, 2, yn) + high, f32),
        pltpu.VMEM((2, 2, yn) + high, f32),
        pltpu.VMEM((2, yn) + high, f32),
        pltpu.VMEM((2, yn) + high, f32),
        pltpu.VMEM((2, yn) + high, f32),
        pltpu.VMEM((2 * yn - 1,) + high, f32),
        dma((2 + len(dot_groups(slots)),)), pltpu.SemaphoreType.REGULAR((max(zn - 2, 1),)),
        pltpu.SemaphoreType.REGULAR, dma, dma((n,)), dma, dma((n,)), dma, dma((2,)), dma, dma((zn - 2,)), dma, dma, dma((6,)),
    ]
    return pl.pallas_call(
        functools.partial(kernel, (yn, zn, slots, share, width)),
        out_shape=pltpu.VMEM(diag.shape, f32),
        in_specs=[pl.BlockSpec(memory_space=pltpu.HBM)] * 4,
        out_specs=pl.BlockSpec(memory_space=pltpu.VMEM),
        scratch_shapes=scratch,
        compiler_params=pltpu.CompilerParams(
            collective_id=0, has_side_effects=True, vmem_limit_bytes=60 * 1024 * 1024
        ),
    )(lhat, ainv, diag, targets.T)


def solution(mesh):
    placed = (
        P(("row", "col"), None, None),
        P(("row", "col"), None, None),
        P("col", "row", None),
        P(("row", "col"), None),
    )
    return jax.shard_map(
        on_device, mesh=mesh, in_specs=placed, out_specs=P("col", "row", None), check_vma=False
    )
```
